32 devices in a mesh: seq: 8 (over z, x), head: 4 (over y, core).
Axes of the slice: x: 2, y: 2, z: 4, core: 2. Of those that a mesh axis runs over, the one named last changes fastest.
Arguments:
- queries: bfloat16 [2048, 4096], P('seq', 'head'), may hold values from -48 to 48
- key_rows: bfloat16 [2048, 4096], P('seq', 'head'), may hold values from -4 to 4
- value_rows: bfloat16 [2048, 4096], P('seq', 'head'), may hold values from -6 to 6
- out_grad: bfloat16 [2048, 2048], P('seq', 'head'), may hold values from -6 to 6
- out_proj: bfloat16 [4096, 2048], P('head'), may hold values from -0.125 to 0.125
- section_table: int32 [32, 3], P('head'), may hold values 0 or 1
- block_active: int32 [8, 3], P('seq'), may hold values 0 or 1
Outputs:
- query_grad: bfloat16 [2048, 4096], P('seq', 'head')
- key_grad: bfloat16 [2048, 4096], P('seq', 'head')
- value_grad: bfloat16 [2048, 4096], P('seq', 'head')
The draws below stay inside these ranges and needn't reach their ends.
All inputs are finite; a program needn't handle non-finite values.
Results may differ from the reference program's by a relative error of at most 0.008.
Values may be sent and summed in bfloat16 or wider, within the bound.
A program may use at most 64 MiB of HBM per device.

```python
import math
from functools import partial
from functools import reduce
import jax
import jax.numpy as jnp
from jax import lax

BLK = 256
HEADS = 32
HDIM = 128
DMODEL = 2048
SECTIONS = 3
NBLOCKS = 8
TOKENS = 2048


def paired_fields(key):
    base_key = jax.random.fold_in(key, 4021)
    field_shape = (TOKENS, HEADS * HDIM)
    key_field = jnp.clip(jax.random.normal(jax.random.fold_in(base_key, 1), field_shape, jnp.float32), -4.0, 4.0)
    query_field = jnp.clip(jax.random.normal(jax.random.fold_in(base_key, 2), field_shape, jnp.float32), -4.0, 4.0)
    return (query_field, key_field)


def draw_queries(key, part):
    return paired_fields(key)[0].astype(jnp.bfloat16)


def draw_key_rows(key, part):
    return paired_fields(key)[1].astype(jnp.bfloat16)


def plant(values, key, smallest, top_value):
    shape = values.shape
    spot = [jax.random.randint(jax.random.fold_in(key, axis), (), 0, shape[axis]) for axis in range(len(shape))]
    values = values.at[tuple(spot)].set(smallest)
    longest = shape.index(max(shape))
    spot[longest] = (spot[longest] + 1) % shape[longest]
    return values.at[tuple(spot)].set(top_value)


def steps_of(rng, shape, shards, smallest, largest):
    factor_of, own = 1.0, jax.random.fold_in(rng, 6)
    for dim, shards_of in shards:
        heights = jnp.exp(jax.random.uniform(jax.random.fold_in(own, dim), (shards_of,), jnp.float32, smallest / len(shards), largest / len(shards)))
        factor_of = factor_of * jnp.repeat(heights, shape[dim] // shards_of).reshape([-1 if axis == dim else 1 for axis in range(len(shape))])
    return factor_of


def centred(own_key, dims, width, bound, split=(), held_as=jnp.bfloat16):
    drawn = width * jax.random.normal(own_key, dims, jnp.float32)
    if split:
        drawn = drawn * steps_of(own_key, dims, split, -0.22, 0.18)
    return jnp.clip(drawn, -bound, bound).astype(held_as)


def setup_inputs(seed: int = 0) -> dict:
    key_list = jax.random.split(jax.random.key(seed), 8)
    return {
        "queries": draw_queries(jax.random.fold_in(key_list[7], 71), 0),
        "key_rows": draw_key_rows(jax.random.fold_in(key_list[7], 71), 0),
        "value_rows": centred(key_list[2], (TOKENS, HEADS * HDIM), 1.0, 6.0, ((0, 8), (1, 4))),
        "out_grad": centred(key_list[3], (TOKENS, DMODEL), 1.0, 6.0, ((0, 8), (1, 4))),
        "out_proj": centred(key_list[4], (HEADS * HDIM, DMODEL), DMODEL ** -0.5, 0.125, ((0, 4),)),
        "section_table": plant((jax.random.randint(key_list[5], (HEADS, SECTIONS), 0, 3) < 2).astype(jnp.int32), jax.random.fold_in(key_list[5], 1), 0, 1),
        "block_active": plant((jax.random.randint(key_list[6], (NBLOCKS, SECTIONS), 0, 4) < 3).astype(jnp.int32), jax.random.fold_in(key_list[6], 1), 0, 1),
    }


def shift_down(blocks, count):
    filler = jnp.zeros((count,) + blocks.shape[1:], blocks.dtype)
    return jnp.concatenate([filler, blocks[:blocks.shape[0] - count]], axis=0)

def shift_up(blocks, count):
    filler = jnp.zeros((count,) + blocks.shape[1:], blocks.dtype)
    return jnp.concatenate([blocks[count:], filler], axis=0)

def to_wide(array):
    return array.astype(jnp.float32)

def narrow(array):
    return lax.optimization_barrier(array.astype(jnp.bfloat16)).astype(jnp.float32)

def head_grads(block_active, operands):
    query_h, key_h, value_h, grad_h, head_flags = operands
    score_scale = 1.0 / math.sqrt(HDIM)
    query_wide = to_wide(query_h)
    key_wide = to_wide(key_h)
    value_wide = to_wide(value_h)
    grad_wide = to_wide(grad_h)
    row_ids = jnp.arange(BLK)
    causal = (row_ids[:, None] >= row_ids[None, :])[None]
    block_ids = jnp.arange(NBLOCKS)
    key_sets = [(key_wide, value_wide, causal, 0)]
    for section_index in range(SECTIONS):
        shift_count = NBLOCKS // 2 ** (section_index + 1)
        usable = (head_flags[section_index] * block_active[:, section_index] > 0) & (block_ids >= shift_count)
        key_sets.append((shift_down(key_wide, shift_count), shift_down(value_wide, shift_count), usable[:, None, None], shift_count))
    logits = []
    for key_entry in key_sets:
        raw_scores = jnp.einsum('bid,bjd->bij', query_wide, key_entry[0]) * score_scale
        logits.append(jnp.where(key_entry[2], raw_scores, -1e+30))
    row_max = reduce(jnp.maximum, [lax.optimization_barrier(jnp.max(logit_set, axis=-1)) for logit_set in logits])
    row_sum = reduce(jnp.add, [lax.optimization_barrier(jnp.sum(jnp.exp(logit_set - row_max[..., None]), axis=-1)) for logit_set in logits])
    log_norm = row_max + jnp.log(row_sum)
    probs_list = [jnp.where(key_entry[2], jnp.exp(logit_set - log_norm[..., None]), 0.0) for logit_set, key_entry in zip(logits, key_sets)]
    weight_list = [narrow(prob_set) for prob_set in probs_list]
    context = reduce(jnp.add, [jnp.einsum('bij,bjd->bid', weight_set, key_entry[1]) for weight_set, key_entry in zip(weight_list, key_sets)])
    row_delta = lax.optimization_barrier(jnp.sum(grad_wide * context, axis=-1))
    query_grad = jnp.zeros_like(query_wide)
    key_grad = jnp.zeros_like(query_wide)
    value_grad = jnp.zeros_like(query_wide)
    for set_index in range(SECTIONS + 1):
        key_part, value_part, allowed, shift_count = key_sets[set_index]
        prob_grad = jnp.einsum('bid,bjd->bij', grad_wide, value_part)
        dlogit = narrow(probs_list[set_index] * (prob_grad - row_delta[..., None]) * score_scale)
        query_grad = query_grad + jnp.einsum('bij,bjd->bid', dlogit, key_part)
        key_term = jnp.einsum('bij,bid->bjd', dlogit, query_wide)
        value_term = jnp.einsum('bij,bid->bjd', weight_list[set_index], grad_wide)
        if set_index > 0:
            key_term = narrow(key_term)
            value_term = narrow(value_term)
        key_grad = key_grad + shift_up(key_term, shift_count)
        value_grad = value_grad + shift_up(value_term, shift_count)
    return (query_grad.astype(jnp.bfloat16), key_grad.astype(jnp.bfloat16), value_grad.astype(jnp.bfloat16))

def by_heads(matrix):
    return matrix.reshape(NBLOCKS, BLK, HEADS, HDIM).transpose(2, 0, 1, 3)

def from_heads(stacked):
    return stacked.transpose(1, 2, 0, 3).reshape(TOKENS, HEADS * HDIM)

def reference(queries, key_rows, value_rows, out_grad, out_proj, section_table, block_active):
    attn_grad = jnp.dot(out_grad, out_proj.T, preferred_element_type=jnp.float32).astype(jnp.bfloat16)
    operands = (by_heads(queries), by_heads(key_rows), by_heads(value_rows), by_heads(attn_grad), section_table)
    query_out, key_out, value_out = lax.map(partial(head_grads, block_active), operands)
    return (from_heads(query_out), from_heads(key_out), from_heads(value_out))
```

```python
import functools
import math

import jax
import jax.numpy as jnp
from jax import lax
from jax.experimental import pallas as pl
from jax.experimental.pallas import tpu as pltpu
from jax.sharding import PartitionSpec as P

HDIM = 128
SECTIONS = 3
SETS = SECTIONS + 1
AHEAD = 2
FAR = 1e30
MESH = pl.DeviceIdType.MESH
BF16 = jnp.bfloat16
F32 = jnp.float32


def dot(a, b, dims):
    return lax.dot_general(a, b, (dims, ((), ())), preferred_element_type=F32)


def kernel(
    count,
    lanes,
    q_hbm,
    k_hbm,
    v_hbm,
    og_hbm,
    proj_hbm,
    table_ref,
    active_ref,
    dq_hbm,
    dk_hbm,
    dv_hbm,
    kv,
    qs,
    gs,
    og,
    proj,
    own,
    stat_out,
    stat_in,
    result,
    kv_load,
    q_load,
    load_sem,
    kv_send,
    kv_recv,
    q_send,
    q_recv,
    og_send,
    og_recv,
    lane_send,
    lane_recv,
    stat_send,
    stat_recv,
    out_sem,
):
    _, heads, _, rows, _ = kv.shape
    width = og.shape[2] // lanes
    scale = 1.0 / math.sqrt(HDIM)
    scale2 = scale / math.log(2.0)
    half, quarter, eighth = count // 2, count // 4, count // 8
    me = lax.axis_index("seq")
    lane = lax.axis_index("head")
    odd = (me // eighth) % 2 == 1
    even = jnp.logical_not(odd)
    up, down = me + quarter, me - quarter
    pair = jnp.where(odd, me - eighth, me + eighth)
    other = jnp.where(odd, me + eighth, me - eighth)
    has_up, has_down = me < count - quarter, me >= quarter
    has_far, has_near = me >= half, me < count - half
    has_both = jnp.logical_and(has_up, has_down)
    odd_or_down = jnp.logical_or(odd, has_down)
    even_or_up = jnp.logical_or(even, has_up)
    odd_and_down = jnp.logical_and(odd, has_down)
    even_and_up = jnp.logical_and(even, has_up)
    has_other = jnp.where(odd, has_up, has_down)
    twin = jnp.where(lane % 2 == 1, lane - 1, lane + 1)
    peers = [lax.rem(lane + 2 * j, lanes) for j in range(1, lanes // 2)]

    def cols(c, size):
        return pl.ds(pl.multiple_of(c * size, size), size)

    def remote(src, dst, send, recv, axis, target):
        return pltpu.make_async_remote_copy(
            src_ref=src,
            dst_ref=dst,
            send_sem=send,
            recv_sem=recv,
            device_id={axis: target},
            device_id_type=MESH,
        )

    def kv_copy(k, source, c, j, target):
        return remote(
            kv.at[j, c, source],
            kv.at[j, c, k],
            kv_send.at[k - 1, j, c],
            kv_recv.at[k - 1, j, c],
            "seq",
            target,
        )

    def q_copy(k, source, c, target):
        return remote(
            qs.at[c, source],
            qs.at[c, k],
            q_send.at[k - 1, c],
            q_recv.at[k - 1, c],
            "seq",
            target,
        )

    def og_copy(k, source, target):
        return remote(
            og.at[source, :, cols(lane, width)],
            og.at[k, :, cols(lane, width)],
            og_send.at[k - 1],
            og_recv.at[k - 1],
            "seq",
            target,
        )

    def lane_copy(k, index, shard, target):
        return remote(
            og.at[k, :, cols(shard, width)],
            og.at[k, :, cols(shard, width)],
            lane_send.at[k, index],
            lane_recv.at[k, shard],
            "head",
            target,
        )

    def stat_copy(k, c, target):
        return remote(
            stat_out.at[c, k - 1],
            stat_in.at[c, k - 1],
            stat_send.at[k - 1, c],
            stat_recv.at[k - 1, c],
            "seq",
            target,
        )

    def load_kv(c, j):
        return pltpu.make_async_copy(
            (k_hbm, v_hbm)[j].at[:, cols(c, HDIM)], kv.at[j, c, 0], kv_load.at[j, c]
        )

    def load_q(c):
        return pltpu.make_async_copy(q_hbm.at[:, cols(c, HDIM)], qs.at[c, 0], q_load.at[c])

    def write(index, c):
        target = (dq_hbm, dk_hbm, dv_hbm)[index]
        return pltpu.make_async_copy(
            result.at[index, c], target.at[:, cols(c, HDIM)], out_sem.at[index, c]
        )

    load_og = pltpu.make_async_copy(og_hbm, og.at[0, :, cols(lane, width)], load_sem.at[0])
    load_proj = pltpu.make_async_copy(proj_hbm, proj, load_sem.at[1])
    load_og.start()

    @pl.loop(0, heads)
    def _(c):
        for j in range(2):
            load_kv(c, j).start()
        load_q(c).start()

    load_proj.start()

    barrier = pltpu.get_barrier_semaphore()
    arrivals = jnp.int32(2 + len(peers))
    for peer in [twin] + peers:
        pl.semaphore_signal(barrier, inc=1, device_id={"head": peer}, device_id_type=MESH)
    pl.semaphore_signal(barrier, inc=1, device_id={"seq": pair}, device_id_type=MESH)
    for present, target in (
        (has_up, up),
        (has_down, down),
        (has_far, me - half),
        (has_near, me + half),
        (has_other, other),
    ):
        arrivals = arrivals + present.astype(jnp.int32)

        @pl.when(present)
        def _():
            pl.semaphore_signal(barrier, inc=1, device_id={"seq": target}, device_id_type=MESH)

    pl.semaphore_wait(barrier, arrivals)

    def gather_start(k):
        for j, peer in enumerate(peers):
            lane_copy(k, 1 + j, lane, peer).start()
        lane_copy(k, 0, lane, twin).start()

    def gather_pass(k):
        for j, peer in enumerate(peers):
            lane_copy(k, 1 + j, peer, lane).wait_recv()
            lane_copy(k, len(peers) + 1 + j, peer, twin).start()

    def gather_end(k):
        lane_copy(k, 0, twin, lane).wait_recv()
        for j in range(len(peers)):
            shard = lax.rem(twin + 2 * (j + 1), lanes)
            lane_copy(k, len(peers) + 1 + j, shard, lane).wait_recv()

    def send_kv(c):
        for j in range(2):
            load_kv(c, j).wait()

            @pl.when(has_up)
            def _():
                kv_copy(2, 0, c, j, up).start()

            @pl.when(even)
            def _():
                kv_copy(3, 0, c, j, pair).start()

    def send_q(c):
        load_q(c).wait()

        @pl.when(has_down)
        def _():
            q_copy(2, 0, c, down).start()

        @pl.when(odd)
        def _():
            q_copy(3, 0, c, pair).start()

    def relay_kv(c):
        for j in range(2):

            @pl.when(has_down)
            def _():
                kv_copy(2, 0, c, j, up).wait_recv()

            @pl.when(has_both)
            def _():
                kv_copy(1, 2, c, j, up).start()

            @pl.when(odd_and_down)
            def _():
                kv_copy(3, 2, c, j, pair).start()

        @pl.when(c + AHEAD < heads)
        def _():
            send_kv(c + AHEAD)

    def relay_q(c):
        @pl.when(has_up)
        def _():
            q_copy(2, 0, c, down).wait_recv()

        @pl.when(has_both)
        def _():
            q_copy(1, 2, c, down).start()

        @pl.when(even_and_up)
        def _():
            q_copy(3, 2, c, pair).start()

    load_og.wait()
    gather_start(0)

    @pl.when(has_down)
    def _():
        og_copy(2, 0, down).start()

    @pl.when(odd)
    def _():
        og_copy(3, 0, pair).start()

    for c in range(AHEAD):
        send_kv(jnp.int32(c))
    here = {1: has_near, 2: has_up, 3: even_or_up}
    reach = {1: has_far, 2: has_down, 3: odd_or_down}
    for k in range(1, SETS):

        @pl.when(jnp.logical_not(reach[k]))
        def _():
            @pl.loop(0, heads)
            def _(c):
                for j in range(2):
                    kv[j, c, k] = jnp.zeros((rows, HDIM), BF16)

        @pl.when(jnp.logical_not(here[k]))
        def _():
            @pl.loop(0, heads)
            def _(c):
                qs[c, k] = jnp.zeros((rows, HDIM), BF16)
                gs[c, k] = jnp.zeros((rows, HDIM), BF16)
                stat_in[c, k - 1] = jnp.full((2, rows), FAR, F32)

    relay_kv(jnp.int32(0))

    def project(k):
        @pl.loop(0, heads // 2)
        def _(t):
            tile = proj[cols(t, 2 * HDIM), :]
            grad = dot(og[k], tile, ((1,), (1,))).astype(BF16)
            gs[2 * t, k] = grad[:, :HDIM]
            gs[2 * t + 1, k] = grad[:, HDIM:]

    gather_pass(0)
    load_proj.wait()
    gather_end(0)
    project(0)

    key_index = lax.broadcasted_iota(jnp.int32, (rows, rows), 0)
    query_index = lax.broadcasted_iota(jnp.int32, (rows, rows), 1)

    def attend(c):
        query, grad = qs[c, 0], gs[c, 0]
        raw = dot(kv[0, c].reshape(SETS * rows, HDIM), query, ((1,), (1,))) * scale2
        prob_grad = dot(kv[1, c].reshape(SETS * rows, HDIM), grad, ((1,), (1,)))
        logits = [raw[k * rows : (k + 1) * rows] for k in range(SETS)]
        prob_grads = [prob_grad[k * rows : (k + 1) * rows] for k in range(SETS)]
        logits[0] = jnp.where(key_index <= query_index, logits[0], -FAR)
        top = jnp.max(logits[0], axis=0, keepdims=True)
        usable = {}
        for k in range(1, SETS):
            usable[k] = jnp.logical_and(
                table_ref[k - 1, c] * active_ref[0, k - 1] > 0, me >= count // 2**k
            )
            best = jnp.max(logits[k], axis=0, keepdims=True)
            top = jnp.maximum(top, best + jnp.where(usable[k], 0.0, -FAR).astype(F32))
        total, weighted, exps = 0.0, 0.0, []
        for k in range(SETS):
            shift = top if k == 0 else top + jnp.where(usable[k], 0.0, FAR).astype(F32)
            exps.append(jnp.exp2(logits[k] - shift))
            total = total + jnp.sum(exps[k], axis=0, keepdims=True)
            weighted = weighted + jnp.sum(exps[k] * prob_grads[k], axis=0, keepdims=True)
        inverse = 1.0 / total
        delta = weighted * inverse
        norm = top + jnp.log2(total)
        for k in range(1, SETS):
            hidden = jnp.where(active_ref[0, k - 1] > 0, 0.0, FAR).astype(F32)
            stat_out[c, k - 1] = jnp.concatenate([norm + hidden, delta], axis=0)

        probs = exps[0] * inverse
        dlogit = (probs * (prob_grads[0] - delta)).astype(BF16)
        own[0, c] = dot(dlogit, query, ((1,), (0,))) * scale
        own[1, c] = dot(probs.astype(BF16), grad, ((1,), (0,)))
        others = jnp.concatenate(
            [(exps[k] * (prob_grads[k] - delta)).astype(BF16) for k in range(1, SETS)], axis=0
        )
        keys = kv[0, c, 1:].reshape(SECTIONS * rows, HDIM)
        far = dot(keys, others, ((0,), (0,))) * inverse
        near = dot(kv[0, c, 0], dlogit, ((0,), (0,)))
        result[0, c] = ((far + near) * scale).T.astype(BF16)

    def tell(c):
        for k, go, span in ((1, has_far, half), (2, has_down, quarter), (3, odd_or_down, eighth)):

            @pl.when(go)
            def _():
                stat_copy(k, c, me - span).start()

        write(0, c).start()

    def collect(c):
        queries = qs[c, 1:].reshape(SECTIONS * rows, HDIM)
        grads = gs[c, 1:].reshape(SECTIONS * rows, HDIM)
        raw = dot(kv[0, c, 0], queries, ((1,), (1,))) * scale2
        prob_grad = dot(kv[1, c, 0], grads, ((1,), (1,)))
        weights, dlogits = [], []
        for k in range(1, SETS):
            part = slice((k - 1) * rows, k * rows)
            hidden = jnp.where(table_ref[k - 1, c] > 0, 0.0, FAR).astype(F32)
            probs = jnp.exp2(raw[:, part] - (stat_in[c, k - 1, 0:1] + hidden))
            weights.append(probs.astype(BF16))
            dlogits.append((probs * (prob_grad[:, part] - stat_in[c, k - 1, 1:2])).astype(BF16))
        key = dot(jnp.concatenate(dlogits, axis=1), queries, ((1,), (0,)))
        value = dot(jnp.concatenate(weights, axis=1), grads, ((1,), (0,)))
        result[1, c] = (own[0, c] + key * scale).astype(BF16)
        result[2, c] = (own[1, c] + value).astype(BF16)

    def finish(c):
        for k, source in ((1, half), (2, quarter), (3, eighth)):

            @pl.when(here[k])
            def _():
                stat_copy(k, c, me + source).wait_recv()

        for k in (1, 3):

            @pl.when(here[k])
            def _():
                q_copy(k, 0, c, me).wait_recv()

        collect(c)
        for index in (1, 2):
            write(index, c).start()

    def arrive(k):
        @pl.when(here[k])
        def _():
            og_copy(k, 0, me).wait_recv()
            if k == 2:

                @pl.when(has_both)
                def _():
                    og_copy(1, 2, down).start()

                @pl.when(even)
                def _():
                    og_copy(3, 2, pair).start()

            gather_start(k)

    def hand_on(k):
        @pl.when(here[k])
        def _():
            gather_pass(k)

    def take(k):
        @pl.when(here[k])
        def _():
            gather_end(k)
            project(k)

    middle = heads // 2

    @pl.loop(0, heads)
    def _(i):
        @pl.when(i < middle)
        def _():
            send_q(2 * i)
            send_q(2 * i + 1)

        for step, action, k in (
            (0, arrive, 2),
            (1, hand_on, 2),
            (1, arrive, 3),
            (2, hand_on, 3),
            (2, arrive, 1),
            (3, hand_on, 1),
        ):

            @pl.when(i == step)
            def _():
                action(k)

        @pl.when(i + 1 < heads)
        def _():
            relay_kv(i + 1)

        @pl.when(jnp.logical_and(i >= 2, i < 2 + middle))
        def _():
            relay_q(2 * (i - 2))
            relay_q(2 * (i - 2) + 1)

        for j in range(2):
            for k in (1, 3):

                @pl.when(reach[k])
                def _():
                    kv_copy(k, 0, i, j, me).wait_recv()

        attend(i)
        tell(i)
        for step, k in ((2, 2), (3, 3), (4, 1)):

            @pl.when(i == step)
            def _():
                take(k)

        first = 2 * (i - middle)

        @pl.when(i >= middle)
        def _():
            @pl.loop(first, jnp.minimum(first + 2, heads - 1))
            def _(c):
                finish(c)

    finish(jnp.int32(heads - 1))

    def drain(k):
        for index in range(lanes - 1):
            lane_copy(k, index, lane, twin).wait_send()

    drain(0)
    for k in range(1, SETS):

        @pl.when(here[k])
        def _():
            drain(k)

    sent = {1: has_both, 2: has_down, 3: jnp.logical_or(odd, has_up)}
    for k in range(1, SETS):

        @pl.when(sent[k])
        def _():
            og_copy(k, 0, pair).wait_send()

    @pl.loop(0, heads)
    def _(c):
        for index in range(3):
            write(index, c).wait()
        for present, copy in (
            (has_both, q_copy(1, 2, c, down)),
            (has_down, q_copy(2, 0, c, down)),
            (jnp.logical_or(odd, has_up), q_copy(3, 0, c, pair)),
            (has_far, stat_copy(1, c, pair)),
            (has_down, stat_copy(2, c, pair)),
            (odd_or_down, stat_copy(3, c, pair)),
        ):

            @pl.when(present)
            def _():
                copy.wait_send()

        for j in range(2):
            for present, k in ((has_both, 1), (has_up, 2), (jnp.logical_or(even, has_down), 3)):

                @pl.when(present)
                def _():
                    kv_copy(k, 0, c, j, up).wait_send()


def publish_kernel(parts, *refs):
    number = (len(refs) - 2) // 2
    sources, targets = refs[:number], refs[number : 2 * number]
    held, sems = refs[2 * number :]
    rows = sources[0].shape[0] // parts
    pieces = [(a, p) for a in range(number) for p in range(parts)]

    def fetch(a, p):
        return pltpu.make_async_copy(
            sources[a].at[pl.ds(p * rows, rows)], held.at[a, p], sems.at[0, a, p]
        )

    def store(a, p):
        return pltpu.make_async_copy(
            held.at[a, p], targets[a].at[pl.ds(p * rows, rows)], sems.at[1, a, p]
        )

    for piece in pieces:
        fetch(*piece).start()
    for piece in pieces:
        fetch(*piece).wait()
        store(*piece).start()
    for piece in pieces:
        store(*piece).wait()


def publish(arrays, parts=2):
    rows, columns = arrays[0].shape
    hbm = pl.BlockSpec(memory_space=pl.ANY)
    number = len(arrays)
    return pl.pallas_call(
        functools.partial(publish_kernel, parts),
        out_shape=[jax.ShapeDtypeStruct(a.shape, a.dtype) for a in arrays],
        in_specs=[hbm] * number,
        out_specs=[hbm] * number,
        scratch_shapes=[
            pltpu.VMEM((number, parts, rows // parts, columns), arrays[0].dtype),
            pltpu.SemaphoreType.DMA((2, number, parts)),
        ],
        compiler_params=pltpu.CompilerParams(vmem_limit_bytes=60 * 2**20),
    )(*arrays)


def body(count, lanes, queries, key_rows, value_rows, out_grad, out_proj, table, active):
    rows, columns = queries.shape
    heads = columns // HDIM
    smem = pl.BlockSpec(memory_space=pltpu.SMEM)
    hbm = pl.BlockSpec(memory_space=pl.ANY)
    dma = pltpu.SemaphoreType.DMA
    grads = pl.pallas_call(
        functools.partial(kernel, count, lanes),
        out_shape=[jax.ShapeDtypeStruct((rows, columns), BF16)] * 3,
        in_specs=[hbm] * 5 + [smem] * 2,
        out_specs=[hbm] * 3,
        scratch_shapes=[
            pltpu.VMEM((2, heads, SETS, rows, HDIM), BF16),
            pltpu.VMEM((heads, SETS, rows, HDIM), BF16),
            pltpu.VMEM((heads, SETS, rows, HDIM), BF16),
            pltpu.VMEM((SETS, rows, out_proj.shape[1]), BF16),
            pltpu.VMEM(out_proj.shape, BF16),
            pltpu.VMEM((2, heads, rows, HDIM), F32),
            pltpu.VMEM((heads, SECTIONS, 2, rows), F32),
            pltpu.VMEM((heads, SECTIONS, 2, rows), F32),
            pltpu.VMEM((3, heads, rows, HDIM), BF16),
            dma((2, heads)),
            dma((heads,)),
            dma((2,)),
            dma((SECTIONS, 2, heads)),
            dma((SECTIONS, 2, heads)),
            dma((SECTIONS, heads)),
            dma((SECTIONS, heads)),
            dma((SECTIONS,)),
            dma((SECTIONS,)),
            dma((SETS, lanes)),
            dma((SETS, lanes)),
            dma((SECTIONS, heads)),
            dma((SECTIONS, heads)),
            dma((3, heads)),
        ],
        compiler_params=pltpu.CompilerParams(
            collective_id=0, has_side_effects=True, vmem_limit_bytes=60 * 2**20
        ),
    )(queries, key_rows, value_rows, out_grad, out_proj, table.T, active)
    return tuple(publish(grads))


def solution(mesh):
    return jax.shard_map(
        functools.partial(body, mesh.shape["seq"], mesh.shape["head"]),
        mesh=mesh,
        in_specs=(
            P("seq", "head"),
            P("seq", "head"),
            P("seq", "head"),
            P("seq", "head"),
            P("head", None),
            P("head", None),
            P("seq", None),
        ),
        out_specs=(P("seq", "head"), P("seq", "head"), P("seq", "head")),
        check_vma=False,
    )
```

```python
import functools
import math

import jax
import jax.numpy as jnp
from jax import lax
from jax.experimental import pallas as pl
from jax.experimental.pallas import tpu as pltpu
from jax.sharding import PartitionSpec as P

HDIM = 128
SECTIONS = 3
SETS = SECTIONS + 1
ASKED = 2
EARLY = 2
FAR = 1e30
MESH = pl.DeviceIdType.MESH
BF16 = jnp.bfloat16
F32 = jnp.float32


def dot(a, b, dims):
    return lax.dot_general(a, b, (dims, ((), ())), preferred_element_type=F32)


def kernel(
    count,
    lanes,
    q_hbm,
    k_hbm,
    v_hbm,
    og_hbm,
    proj_hbm,
    table_ref,
    active_ref,
    dq_ref,
    dk_ref,
    dv_ref,
    kv,
    qs,
    gs,
    og,
    proj,
    own,
    stat_out,
    stat_in,
    part_own,
    part_out,
    part_in,
    stat_own,
    held,
    term,
    back,
    kv_load,
    q_load,
    load_sem,
    kv_send,
    kv_recv,
    q_send,
    q_recv,
    og_send,
    og_recv,
    lane_send,
    lane_recv,
    stat_send,
    stat_recv,
    part_send,
    part_recv,
    term_send,
    term_recv,
):
    _, heads, _, rows, _ = kv.shape
    width = og.shape[2] // lanes
    piece = rows // 2
    keyed = heads - ASKED
    scale = 1.0 / math.sqrt(HDIM)
    scale2 = scale / math.log(2.0)
    half, quarter, eighth = count // 2, count // 4, count // 8
    me = lax.axis_index("seq")
    lane = lax.axis_index("head")
    odd = (me // eighth) % 2 == 1
    even = jnp.logical_not(odd)
    up, down = me + quarter, me - quarter
    pair = jnp.where(odd, me - eighth, me + eighth)
    other = jnp.where(odd, me + eighth, me - eighth)
    has_up, has_down = me < count - quarter, me >= quarter
    has_far, has_near = me >= half, me < count - half
    has_both = jnp.logical_and(has_up, has_down)
    odd_or_down = jnp.logical_or(odd, has_down)
    even_or_up = jnp.logical_or(even, has_up)
    odd_and_down = jnp.logical_and(odd, has_down)
    even_and_up = jnp.logical_and(even, has_up)
    has_other = jnp.where(odd, has_up, has_down)
    twin = jnp.where(lane % 2 == 1, lane - 1, lane + 1)
    peers = [lax.rem(lane + 2 * j, lanes) for j in range(1, lanes // 2)]

    def cols(c, size):
        return pl.ds(pl.multiple_of(c * size, size), size)

    def remote(src, dst, send, recv, axis, target):
        return pltpu.make_async_remote_copy(
            src_ref=src,
            dst_ref=dst,
            send_sem=send,
            recv_sem=recv,
            device_id={axis: target},
            device_id_type=MESH,
        )

    def kv_copy(k, source, c, target):
        return remote(
            kv.at[:, c, source],
            kv.at[:, c, k],
            kv_send.at[k - 1],
            kv_recv.at[k - 1, c],
            "seq",
            target,
        )

    def q_copy(k, source, c, target):
        return remote(
            qs.at[c, source],
            qs.at[c, k],
            q_send.at[k - 1],
            q_recv.at[k - 1, c],
            "seq",
            target,
        )

    def og_copy(k, source, p, target):
        part = pl.ds(p * piece, piece)
        return remote(
            og.at[source, part, cols(lane, width)],
            og.at[k, part, cols(lane, width)],
            og_send.at[k - 1],
            og_recv.at[k - 1, p],
            "seq",
            target,
        )

    def lane_copy(k, shard, p, target):
        part = og.at[k, pl.ds(p * piece, piece), cols(shard, width)]
        return remote(
            part, part, lane_send.at[k], lane_recv.at[k, p, shard], "head", target
        )

    def part_copy(k, c, target):
        return remote(
            part_out.at[c - keyed, k - 1],
            part_in.at[c - keyed, k - 1],
            part_send.at[k - 1],
            part_recv.at[k - 1, c - keyed],
            "seq",
            target,
        )

    def term_copy(k, c, target):
        return remote(
            term.at[c - keyed, k - 1],
            back.at[c - keyed, k - 1],
            term_send.at[k - 1],
            term_recv.at[k - 1, c - keyed],
            "seq",
            target,
        )

    def stat_copy(k, c, target):
        return remote(
            stat_out.at[c, k - 1],
            stat_in.at[c, k - 1],
            stat_send.at[k - 1],
            stat_recv.at[k - 1, c],
            "seq",
            target,
        )

    def load_kv(c, j):
        return pltpu.make_async_copy(
            (k_hbm, v_hbm)[j].at[:, cols(c, HDIM)], kv.at[j, c, 0], kv_load.at[j, c]
        )

    def load_q(c):
        return pltpu.make_async_copy(q_hbm.at[:, cols(c, HDIM)], qs.at[c, 0], q_load.at[c])

    barrier = pltpu.get_barrier_semaphore()
    arrivals = jnp.int32(2 + len(peers))
    for peer in [twin] + peers:
        pl.semaphore_signal(barrier, inc=1, device_id={"head": peer}, device_id_type=MESH)
    pl.semaphore_signal(barrier, inc=1, device_id={"seq": pair}, device_id_type=MESH)
    for present, target in (
        (has_up, up),
        (has_down, down),
        (has_far, me - half),
        (has_near, me + half),
        (has_other, other),
    ):
        arrivals = arrivals + present.astype(jnp.int32)

        @pl.when(present)
        def _():
            pl.semaphore_signal(barrier, inc=1, device_id={"seq": target}, device_id_type=MESH)

    load_og = pltpu.make_async_copy(og_hbm, og.at[0, :, cols(lane, width)], load_sem.at[0])

    def load_proj(t):
        part = pl.ds(t * 2 * HDIM, 2 * HDIM)
        return pltpu.make_async_copy(proj_hbm.at[part], proj.at[part], load_sem.at[1 + t])

    load_og.start()
    for c in range(EARLY):
        for j in range(2):
            load_kv(c, j).start()

    pl.semaphore_wait(barrier, arrivals)

    def gather_start(k, p):
        for peer in peers:
            lane_copy(k, lane, p, peer).start()
        lane_copy(k, lane, p, twin).start()

    def gather_pass(k):
        for p in range(2):
            for peer in peers:
                lane_copy(k, peer, p, lane).wait_recv()
                lane_copy(k, peer, p, twin).start()

    def gather_end(k):
        for p in range(2):
            lane_copy(k, twin, p, lane).wait_recv()
            for j in range(len(peers)):
                shard = lax.rem(twin + 2 * (j + 1), lanes)
                lane_copy(k, shard, p, lane).wait_recv()

    loaded = set()

    def ready(c):
        if c not in loaded:
            loaded.add(c)
            for copy in [load_q(c)] if c < heads else map(load_proj, range(heads // 2)):
                copy.wait()

    def send_kv(c):
        for j in range(2):
            load_kv(c, j).wait()

        @pl.when(has_up)
        def _():
            kv_copy(2, 0, c, up).start()

        @pl.when(even)
        def _():
            kv_copy(3, 0, c, pair).start()

    def send_q(c):
        ready(c)

        @pl.when(has_down)
        def _():
            q_copy(2, 0, c, down).start()

    def side_q(c):
        ready(c)

        @pl.when(odd)
        def _():
            q_copy(3, 0, c, pair).start()

    def relay_kv(c):
        @pl.when(has_down)
        def _():
            kv_copy(2, 0, c, up).wait_recv()

        @pl.when(has_both)
        def _():
            kv_copy(1, 2, c, up).start()

        @pl.when(odd_and_down)
        def _():
            kv_copy(3, 2, c, pair).start()

    def relay_q(c):
        @pl.when(has_up)
        def _():
            q_copy(2, 0, c, down).wait_recv()

        @pl.when(has_both)
        def _():
            q_copy(1, 2, c, down).start()

        @pl.when(even_and_up)
        def _():
            q_copy(3, 2, c, pair).start()

    load_og.wait()
    for p in range(2):
        gather_start(0, p)

        @pl.when(has_down)
        def _():
            og_copy(2, 0, p, down).start()

        @pl.when(odd)
        def _():
            og_copy(3, 0, p, pair).start()

    for c in range(EARLY, heads):
        for j in range(2):
            load_kv(c, j).start()

    for c in range(heads):
        load_q(c).start()

    here = {0: me >= 0, 1: has_near, 2: has_up, 3: even_or_up}
    reach = {1: has_far, 2: has_down, 3: odd_or_down}
    for k in range(1, SETS):

        @pl.when(jnp.logical_not(reach[k]))
        def _():
            @pl.loop(0, keyed)
            def _(c):
                for j in range(2):
                    kv[j, c, k] = jnp.zeros((rows, HDIM), BF16)

            for c in range(ASKED):
                part_in[c, k - 1] = jnp.full((3, rows), -FAR, F32)

        @pl.when(jnp.logical_not(here[k]))
        def _():
            @pl.loop(0, heads)
            def _(c):
                qs[c, k] = jnp.zeros((rows, HDIM), BF16)
                gs[c, k] = jnp.zeros((rows, HDIM), BF16)
                stat_in[c, k - 1] = jnp.full((2, rows), FAR, F32)

    for k, present in ((1, has_both), (2, has_down), (3, jnp.logical_or(odd, has_up))):

        @pl.when(jnp.logical_not(present))
        def _():
            for c in range(ASKED):
                back[c, k - 1] = jnp.zeros((HDIM, rows), BF16)

    def project(k, low, high):
        @pl.loop(low // 2, high // 2)
        def _(t):
            tile = proj[cols(t, 2 * HDIM), :]
            grad = dot(og[k], tile, ((1,), (1,))).astype(BF16)
            gs[2 * t, k] = grad[:, :HDIM]
            gs[2 * t + 1, k] = grad[:, HDIM:]

    key_index = lax.broadcasted_iota(jnp.int32, (rows, rows), 0)
    query_index = lax.broadcasted_iota(jnp.int32, (rows, rows), 1)

    def attend(c):
        ready(c)
        for k in (1, 3):

            @pl.when(reach[k])
            def _():
                kv_copy(k, 0, c, me).wait_recv()

        query, grad = qs[c, 0], gs[c, 0]
        raw = dot(kv[0, c].reshape(SETS * rows, HDIM), query, ((1,), (1,))) * scale2
        prob_grad = dot(kv[1, c].reshape(SETS * rows, HDIM), grad, ((1,), (1,)))
        logits = [raw[k * rows : (k + 1) * rows] for k in range(SETS)]
        prob_grads = [prob_grad[k * rows : (k + 1) * rows] for k in range(SETS)]
        logits[0] = jnp.where(key_index <= query_index, logits[0], -FAR)
        top = jnp.max(logits[0], axis=0, keepdims=True)
        usable = {}
        for k in range(1, SETS):
            usable[k] = jnp.logical_and(
                table_ref[k - 1, c] * active_ref[0, k - 1] > 0, me >= count // 2**k
            )
            best = jnp.max(logits[k], axis=0, keepdims=True)
            top = jnp.maximum(top, best + jnp.where(usable[k], 0.0, -FAR).astype(F32))
        total, weighted, exps = 0.0, 0.0, []
        for k in range(SETS):
            shift = top if k == 0 else top + jnp.where(usable[k], 0.0, FAR).astype(F32)
            exps.append(jnp.exp2(logits[k] - shift))
            total = total + jnp.sum(exps[k], axis=0, keepdims=True)
            weighted = weighted + jnp.sum(exps[k] * prob_grads[k], axis=0, keepdims=True)
        inverse = 1.0 / total
        delta = weighted * inverse
        norm = top + jnp.log2(total)
        for k in range(1, SETS):
            hidden = jnp.where(active_ref[0, k - 1] > 0, 0.0, FAR).astype(F32)
            stat_out[c, k - 1] = jnp.concatenate([norm + hidden, delta], axis=0)

        probs = exps[0] * inverse
        dlogit = (probs * (prob_grads[0] - delta)).astype(BF16)
        own[0, c] = dot(dlogit, query, ((1,), (0,))) * scale
        own[1, c] = dot(probs.astype(BF16), grad, ((1,), (0,)))
        others = jnp.concatenate(
            [(exps[k] * (prob_grads[k] - delta)).astype(BF16) for k in range(1, SETS)], axis=0
        )
        keys = kv[0, c, 1:].reshape(SECTIONS * rows, HDIM)
        far = dot(keys, others, ((0,), (0,))) * inverse
        near = dot(kv[0, c, 0], dlogit, ((0,), (0,)))
        dq_ref[:, cols(c, HDIM)] = ((far + near) * scale).T.astype(BF16)
        tell(c)

    def tell(c):
        for k, go, span in ((1, has_far, half), (2, has_down, quarter), (3, odd_or_down, eighth)):

            @pl.when(go)
            def _():
                stat_copy(k, c, me - span).start()

    def collect(c):
        queries = qs[c, 1:].reshape(SECTIONS * rows, HDIM)
        grads = gs[c, 1:].reshape(SECTIONS * rows, HDIM)
        raw = dot(kv[0, c, 0], queries, ((1,), (1,))) * scale2
        prob_grad = dot(kv[1, c, 0], grads, ((1,), (1,)))
        weights, dlogits = [], []
        for k in range(1, SETS):
            part = slice((k - 1) * rows, k * rows)
            hidden = jnp.where(table_ref[k - 1, c] > 0, 0.0, FAR).astype(F32)
            probs = jnp.exp2(raw[:, part] - (stat_in[c, k - 1, 0:1] + hidden))
            weights.append(probs.astype(BF16))
            dlogits.append((probs * (prob_grad[:, part] - stat_in[c, k - 1, 1:2])).astype(BF16))
        key = dot(jnp.concatenate(dlogits, axis=1), queries, ((1,), (0,)))
        value = dot(jnp.concatenate(weights, axis=1), grads, ((1,), (0,)))
        dk_ref[:, cols(c, HDIM)] = (own[0, c] + key * scale).astype(BF16)
        dv_ref[:, cols(c, HDIM)] = (own[1, c] + value).astype(BF16)

    def finish(c):
        for k, source in ((1, half), (2, quarter), (3, eighth)):

            @pl.when(here[k])
            def _():
                stat_copy(k, c, me + source).wait_recv()

        for k in (1, 3):

            @pl.when(here[k])
            def _():
                q_copy(k, 0, c, me).wait_recv()

        collect(c)

    def arrive(k, p):
        @pl.when(here[k])
        def _():
            og_copy(k, 0, p, me).wait_recv()
            if k == 2:

                @pl.when(has_both)
                def _():
                    og_copy(1, 2, p, down).start()

                @pl.when(even)
                def _():
                    og_copy(3, 2, p, pair).start()

            gather_start(k, p)

    def hand_on(k):
        @pl.when(here[k])
        def _():
            gather_pass(k)

    def take(k, low=0, high=heads):
        ready(heads)

        @pl.when(here[k])
        def _():
            gather_end(k)
            project(k, low, high)

    def some(k):
        take(k, keyed, heads)

    def rest(k):
        @pl.when(here[k])
        def _():
            project(k, 0, keyed)

    def ask(c):
        for k in (1, 3):

            @pl.when(here[k])
            def _():
                q_copy(k, 0, c, me).wait_recv()

        for j in range(2):
            load_kv(c, j).wait()
        raw = dot(kv[0, c, 0], qs[c].reshape(SETS * rows, HDIM), ((1,), (1,))) * scale2
        prob_grad = dot(kv[1, c, 0], gs[c].reshape(SETS * rows, HDIM), ((1,), (1,)))
        for k in range(SETS):
            part = slice(k * rows, (k + 1) * rows)
            logits = raw[:, part]
            if k == 0:
                logits = jnp.where(key_index <= query_index, logits, -FAR)
            top = jnp.max(logits, axis=0, keepdims=True)
            exps = jnp.exp2(logits - top)
            total = jnp.sum(exps, axis=0, keepdims=True)
            weighted = jnp.sum(exps * prob_grad[:, part], axis=0, keepdims=True)
            if k == 0:
                part_own[c - keyed] = jnp.concatenate([top, total, weighted], axis=0)
            else:
                top = top + jnp.where(table_ref[k - 1, c] > 0, 0.0, -FAR).astype(F32)
                part_out[c - keyed, k - 1] = jnp.concatenate([top, total, weighted], axis=0)
        for k, span in ((1, half), (2, quarter), (3, eighth)):

            @pl.when(here[k])
            def _():
                part_copy(k, c, me + span).start()

    def combine(c):
        for k in range(1, SETS):

            @pl.when(reach[k])
            def _():
                part_copy(k, c, me).wait_recv()

        h = c - keyed
        tops, parts = [part_own[h, 0:1]], [(part_own[h, 1:2], part_own[h, 2:3])]
        for k in range(1, SETS):
            usable = jnp.logical_and(active_ref[0, k - 1] > 0, me >= count // 2**k)
            hidden = jnp.where(usable, 0.0, -FAR).astype(F32)
            tops.append(part_in[h, k - 1, 0:1] + hidden)
            sums = part_in[h, k - 1]
            parts.append((jnp.where(usable, sums[1:2], 0.0), jnp.where(usable, sums[2:3], 0.0)))
        top = functools.reduce(jnp.maximum, tops)
        shares = [jnp.exp2(x - top) for x in tops]
        total = sum(share * part[0] for share, part in zip(shares, parts))
        delta = sum(share * part[1] for share, part in zip(shares, parts)) / total
        norm = top + jnp.log2(total)
        stat_own[h] = jnp.concatenate([norm, delta], axis=0)
        for k in range(1, SETS):
            hidden = jnp.where(active_ref[0, k - 1] > 0, 0.0, FAR).astype(F32)
            stat_out[c, k - 1] = jnp.concatenate([norm + hidden, delta], axis=0)
        tell(c)

    def answer(c):
        for k, span in ((1, half), (2, quarter), (3, eighth)):

            @pl.when(here[k])
            def _():
                stat_copy(k, c, me + span).wait_recv()

        h = c - keyed
        queries = qs[c].reshape(SETS * rows, HDIM)
        grads = gs[c].reshape(SETS * rows, HDIM)
        raw = dot(kv[0, c, 0], queries, ((1,), (1,))) * scale2
        prob_grad = dot(kv[1, c, 0], grads, ((1,), (1,)))
        weights, dlogits = [], []
        for k in range(SETS):
            part = slice(k * rows, (k + 1) * rows)
            logits = raw[:, part]
            if k == 0:
                logits = jnp.where(key_index <= query_index, logits, -FAR)
                norm, delta = stat_own[h, 0:1], stat_own[h, 1:2]
            else:
                hidden = jnp.where(table_ref[k - 1, c] > 0, 0.0, FAR).astype(F32)
                norm, delta = stat_in[c, k - 1, 0:1] + hidden, stat_in[c, k - 1, 1:2]
            probs = jnp.exp2(logits - norm)
            weights.append(probs.astype(BF16))
            dlogits.append((probs * (prob_grad[:, part] - delta)).astype(BF16))
        dlogit = jnp.concatenate(dlogits, axis=1)
        terms = dot(kv[0, c, 0], dlogit, ((0,), (0,))) * scale
        held[h] = terms[:, :rows]
        for k in range(1, SETS):
            term[h, k - 1] = terms[:, k * rows : (k + 1) * rows].astype(BF16)

        @pl.when(has_near)
        def _():
            term_copy(1, c, up).start()

        @pl.when(even_or_up)
        def _():
            term_copy(3, c, pair).start()

        dk_ref[:, cols(c, HDIM)] = (dot(dlogit, queries, ((1,), (0,))) * scale).astype(BF16)
        weight = jnp.concatenate(weights, axis=1)
        dv_ref[:, cols(c, HDIM)] = dot(weight, grads, ((1,), (0,))).astype(BF16)

    def merge(c):
        h = c - keyed

        @pl.when(has_both)
        def _():
            term_copy(1, c, me).wait_recv()

        @pl.when(jnp.logical_or(odd, has_up))
        def _():
            term_copy(3, c, me).wait_recv()

        @pl.when(has_up)
        def _():
            side = jnp.where(even, back[h, 2].astype(F32), 0.0)
            total = term[h, 1].astype(F32) + back[h, 0].astype(F32) + side
            term[h, 1] = total.astype(BF16)
            term_copy(2, c, up).start()

    def close(c):
        h = c - keyed

        @pl.when(has_down)
        def _():
            term_copy(2, c, me).wait_recv()

        side = jnp.where(odd, back[h, 2].astype(F32), 0.0)
        total = held[h] + back[h, 1].astype(F32) + side
        dq_ref[:, cols(c, HDIM)] = total.T.astype(BF16)

    plan = []
    for low, high, timed in (
        (
            0,
            keyed,
            (
                (side_q, -91.11, 1.92),
                (send_kv, -51.98, 9.29),
                (send_q, -2.16, 0.60),
                (relay_kv, 11.21, 6.52),
                (relay_q, 22.85, 7.09),
                (attend, 24.91, 6.64),
                (finish, 51.12, 10.08),
            ),
        ),
        (
            keyed,
            heads,
            (
                (send_q, -45.24, 38.26),
                (side_q, -7.31, 23.83),
                (relay_q, 2.36, 0.25),
                (ask, 33.73, 0.72),
                (combine, 39.90, 0.59),
                (answer, 51.27, 0.22),
                (merge, 58.78, 18.74),
                (close, 119.40, 149.97),
            ),
        ),
    ):
        for action, start, step in timed:
            for c in range(low, high):
                plan.append((start + step * (c - low), functools.partial(action, c)))

    for due, action, *where in (
        (-35.11, arrive, 2, 0),
        (-27.21, arrive, 2, 1),
        (-24.12, arrive, 3, 0),
        (-8.84, arrive, 1, 0),
        (-0.76, hand_on, 2),
        (4.43, arrive, 3, 1),
        (8.56, hand_on, 0),
        (19.32, arrive, 1, 1),
        (22.67, take, 2),
        (22.76, take, 0),
        (23.92, hand_on, 3),
        (26.91, some, 3),
        (28.55, hand_on, 1),
        (31.47, rest, 3),
        (31.58, some, 1),
        (37.51, rest, 1),
    ):
        plan.append((due, functools.partial(action, *where)))

    for t in range(heads // 2):
        plan.append((-30.0 + t * 0.001, load_proj(t).start))

    plan.sort(key=lambda entry: entry[0])
    for _, action in plan:
        action()

    def drain(present, ref, sem):
        @pl.when(present)
        def _():
            pltpu.make_async_copy(ref, ref, sem).wait()

    always = me >= 0
    odd_or_up = jnp.logical_or(odd, has_up)
    drain(always, og.at[0, :, pl.ds(0, (lanes - 1) * width)], lane_send.at[0])
    for k, kv_sent, q_sent, term_sent in (
        (1, has_both, has_both, has_near),
        (2, has_up, has_down, has_up),
        (3, jnp.logical_or(even, has_down), odd_or_up, even_or_up),
    ):
        drain(here[k], og.at[k, :, pl.ds(0, (lanes - 1) * width)], lane_send.at[k])
        drain(q_sent, og.at[0, :, pl.ds(0, width)], og_send.at[k - 1])
        drain(q_sent, qs.at[:, k], q_send.at[k - 1])
        drain(kv_sent, kv.at[:, pl.ds(0, keyed), k], kv_send.at[k - 1])
        drain(reach[k], stat_out.at[:, k - 1], stat_send.at[k - 1])
        drain(here[k], part_out.at[:, k - 1], part_send.at[k - 1])
        drain(term_sent, term.at[:, k - 1], term_send.at[k - 1])


def publish_kernel(*refs):
    number = (len(refs) - 1) // 2
    copies = [
        pltpu.make_async_copy(refs[a], refs[number + a], refs[-1].at[a]) for a in range(number)
    ]
    for copy in copies:
        copy.start()
    for copy in copies:
        copy.wait()


def publish(arrays):
    number = len(arrays)
    held = [pltpu.with_memory_space_constraint(a, pltpu.VMEM) for a in arrays]
    return pl.pallas_call(
        publish_kernel,
        out_shape=[jax.ShapeDtypeStruct(a.shape, a.dtype) for a in arrays],
        in_specs=[pl.BlockSpec(memory_space=pltpu.VMEM)] * number,
        out_specs=[pl.BlockSpec(memory_space=pl.ANY)] * number,
        scratch_shapes=[pltpu.SemaphoreType.DMA((number,))],
        compiler_params=pltpu.CompilerParams(vmem_limit_bytes=2**20),
    )(*held)


def body(count, lanes, queries, key_rows, value_rows, out_grad, out_proj, table, active):
    rows, columns = queries.shape
    heads = columns // HDIM
    smem = pl.BlockSpec(memory_space=pltpu.SMEM)
    vmem = pl.BlockSpec(memory_space=pltpu.VMEM)
    hbm = pl.BlockSpec(memory_space=pl.ANY)
    dma = pltpu.SemaphoreType.DMA
    grads = pl.pallas_call(
        functools.partial(kernel, count, lanes),
        out_shape=[pltpu.VMEM((rows, columns), BF16)] * 3,
        in_specs=[hbm] * 5 + [smem] * 2,
        out_specs=[vmem] * 3,
        scratch_shapes=[
            pltpu.VMEM((2, heads, SETS, rows, HDIM), BF16),
            pltpu.VMEM((heads, SETS, rows, HDIM), BF16),
            pltpu.VMEM((heads, SETS, rows, HDIM), BF16),
            pltpu.VMEM((SETS, rows, out_proj.shape[1]), BF16),
            pltpu.VMEM(out_proj.shape, BF16),
            pltpu.VMEM((2, heads, rows, HDIM), F32),
            pltpu.VMEM((heads, SECTIONS, 2, rows), F32),
            pltpu.VMEM((heads, SECTIONS, 2, rows), F32),
            pltpu.VMEM((ASKED, 3, rows), F32),
            pltpu.VMEM((ASKED, SECTIONS, 3, rows), F32),
            pltpu.VMEM((ASKED, SECTIONS, 3, rows), F32),
            pltpu.VMEM((ASKED, 2, rows), F32),
            pltpu.VMEM((ASKED, HDIM, rows), F32),
            pltpu.VMEM((ASKED, SECTIONS, HDIM, rows), BF16),
            pltpu.VMEM((ASKED, SECTIONS, HDIM, rows), BF16),
            dma((2, heads)),
            dma((heads,)),
            dma((1 + heads // 2,)),
            dma((SECTIONS,)),
            dma((SECTIONS, heads)),
            dma((SECTIONS,)),
            dma((SECTIONS, heads)),
            dma((SECTIONS,)),
            dma((SECTIONS, 2)),
            dma((SETS,)),
            dma((SETS, 2, lanes)),
            dma((SECTIONS,)),
            dma((SECTIONS, heads)),
            dma((SECTIONS,)),
            dma((SECTIONS, ASKED)),
            dma((SECTIONS,)),
            dma((SECTIONS, ASKED)),
        ],
        compiler_params=pltpu.CompilerParams(
            collective_id=0, has_side_effects=True, vmem_limit_bytes=60 * 2**20
        ),
    )(queries, key_rows, value_rows, out_grad, out_proj, table.T, active)
    return tuple(publish(grads))


def solution(mesh):
    return jax.shard_map(
        functools.partial(body, mesh.shape["seq"], mesh.shape["head"]),
        mesh=mesh,
        in_specs=(
            P("seq", "head"),
            P("seq", "head"),
            P("seq", "head"),
            P("seq", "head"),
            P("head", None),
            P("head", None),
            P("seq", None),
        ),
        out_specs=(P("seq", "head"), P("seq", "head"), P("seq", "head")),
        check_vma=False,
    )
```

```python
import functools
import math

import jax
import jax.numpy as jnp
from jax import lax
from jax.experimental import pallas as pl
from jax.experimental.pallas import tpu as pltpu
from jax.sharding import PartitionSpec as P

HDIM = 128
SECTIONS = 3
SETS = SECTIONS + 1
ASKED = 2
EARLY = 2
FAR = 1e30
MESH = pl.DeviceIdType.MESH
BF16 = jnp.bfloat16
F32 = jnp.float32


def dot(a, b, dims):
    return lax.dot_general(a, b, (dims, ((), ())), preferred_element_type=F32)


def kernel(
    count,
    lanes,
    q_hbm,
    k_hbm,
    v_hbm,
    og_hbm,
    proj_hbm,
    table_hbm,
    active_hbm,
    dq_ref,
    dk_ref,
    dv_ref,
    kv,
    qs,
    gs,
    og,
    proj,
    own,
    stat_out,
    stat_in,
    part_own,
    part_out,
    part_in,
    stat_own,
    held,
    term,
    back,
    table_ref,
    active_ref,
    load_sem,
    kv_send,
    kv_recv,
    q_send,
    q_recv,
    og_send,
    og_recv,
    lane_send,
    peer_recv,
    twin_recv,
    stat_send,
    stat_recv,
    part_send,
    part_recv,
    term_send,
    term_recv,
):
    _, heads, _, rows, _ = kv.shape
    width = og.shape[2] // lanes
    piece = rows // 2
    keyed = heads - ASKED
    scale = 1.0 / math.sqrt(HDIM)
    scale2 = scale / math.log(2.0)
    half, quarter, eighth = count // 2, count // 4, count // 8
    me = lax.axis_index("seq")
    lane = lax.axis_index("head")
    odd = (me // eighth) % 2 == 1
    even = jnp.logical_not(odd)
    up, down = me + quarter, me - quarter
    pair = jnp.where(odd, me - eighth, me + eighth)
    other = jnp.where(odd, me + eighth, me - eighth)
    has_up, has_down = me < count - quarter, me >= quarter
    has_far, has_near = me >= half, me < count - half
    has_both = jnp.logical_and(has_up, has_down)
    odd_or_down = jnp.logical_or(odd, has_down)
    even_or_up = jnp.logical_or(even, has_up)
    odd_and_down = jnp.logical_and(odd, has_down)
    even_and_up = jnp.logical_and(even, has_up)
    has_other = jnp.where(odd, has_up, has_down)
    twin = jnp.where(lane % 2 == 1, lane - 1, lane + 1)
    peers = [lax.rem(lane + 2 * j, lanes) for j in range(1, lanes // 2)]

    def cols(c, size):
        return pl.ds(pl.multiple_of(c * size, size), size)

    def remote(src, dst, send, recv, axis, target):
        return pltpu.make_async_remote_copy(
            src_ref=src,
            dst_ref=dst,
            send_sem=send,
            recv_sem=recv,
            device_id={axis: target},
            device_id_type=MESH,
        )

    def kv_copy(k, source, c, target):
        return remote(
            kv.at[:, c, source],
            kv.at[:, c, k],
            kv_send.at[k - 1],
            kv_recv.at[k - 1, c],
            "seq",
            target,
        )

    def q_copy(k, source, g, target):
        duo = pl.ds(2 * g, 2)
        return remote(
            qs.at[duo, source],
            qs.at[duo, k],
            q_send.at[k - 1],
            q_recv.at[k - 1, g],
            "seq",
            target,
        )

    def og_copy(k, source, p, target):
        part = pl.ds(p * piece, piece)
        return remote(
            og.at[source, part, cols(lane, width)],
            og.at[k, part, cols(lane, width)],
            og_send.at[k - 1],
            og_recv.at[k - 1, p],
            "seq",
            target,
        )

    def peer_copy(k, j, shard, p, target):
        part = og.at[k, pl.ds(p * piece, piece), cols(shard, width)]
        return remote(part, part, lane_send.at[k], peer_recv.at[k, p, j], "head", target)

    def twin_copy(k, shard, p):
        part = og.at[k, pl.ds(p * piece, piece), cols(shard, width)]
        return remote(part, part, lane_send.at[k], twin_recv.at[k], "head", twin)

    def part_copy(k, target):
        return remote(
            part_out.at[:, k - 1],
            part_in.at[:, k - 1],
            part_send.at[k - 1],
            part_recv.at[k - 1],
            "seq",
            target,
        )

    def term_copy(k, c, target):
        return remote(
            term.at[c - keyed, k - 1],
            back.at[c - keyed, k - 1],
            term_send.at[k - 1],
            term_recv.at[k - 1, c - keyed],
            "seq",
            target,
        )

    groups = [(0, keyed - 2), (keyed - 2, keyed - 1), (keyed - 1, keyed), (keyed, heads)]

    def group_of(c):
        return [low <= c < high for low, high in groups].index(True)

    def stat_copy(k, group, target):
        low, high = groups[group]
        some_heads = pl.ds(low, high - low)
        return remote(
            stat_out.at[some_heads, k - 1],
            stat_in.at[some_heads, k - 1],
            stat_send.at[k - 1],
            stat_recv.at[k - 1, group],
            "seq",
            target,
        )

    barrier = pltpu.get_barrier_semaphore()
    arrivals = jnp.int32(2 + len(peers))
    for peer in [twin] + peers:
        pl.semaphore_signal(barrier, inc=1, device_id={"head": peer}, device_id_type=MESH)
    pl.semaphore_signal(barrier, inc=1, device_id={"seq": pair}, device_id_type=MESH)
    for present, target in (
        (has_up, up),
        (has_down, down),
        (has_far, me - half),
        (has_near, me + half),
        (has_other, other),
    ):
        arrivals = arrivals + present.astype(jnp.int32)

        @pl.when(present)
        def _():
            pl.semaphore_signal(barrier, inc=1, device_id={"seq": target}, device_id_type=MESH)

    load_og = pltpu.make_async_copy(og_hbm, og.at[0, :, cols(lane, width)], load_sem.at[0])

    def load_kv(c):
        for j, source in enumerate((k_hbm, v_hbm)):
            pltpu.make_async_copy(
                source.at[:, cols(c, HDIM)],
                kv.at[j, c, 0],
                load_sem.at[1 if c < EARLY else 2],
            ).start()

    load_og.start()
    for c in range(EARLY):
        load_kv(c)

    pl.semaphore_wait(barrier, arrivals)

    def gather_start(k, p):
        for j, peer in enumerate(peers):
            peer_copy(k, j, lane, p, peer).start()
        twin_copy(k, lane, p).start()

    def gather_pass(k):
        for p in range(2):
            for j in range(len(peers)):
                shard = lax.rem(lane + lanes - 2 * (j + 1), lanes)
                peer_copy(k, j, shard, p, lane).wait_recv()
                twin_copy(k, shard, p).start()

    def gather_end(k):
        settle(og.at[k, :, pl.ds(0, lanes // 2 * width)], twin_recv.at[k]).wait()

    def send_kv(c):
        ready("early" if c < EARLY else "late")

        @pl.when(has_up)
        def _():
            kv_copy(2, 0, c, up).start()

        @pl.when(even)
        def _():
            kv_copy(3, 0, c, pair).start()

    def send_q(c):
        ready("query")

        @pl.when(has_down)
        def _():
            q_copy(2, 0, c, down).start()

    def side_q(c):
        ready("query")

        @pl.when(odd)
        def _():
            q_copy(3, 0, c, pair).start()

    def relay_kv(c):
        @pl.when(has_down)
        def _():
            kv_copy(2, 0, c, up).wait_recv()

        @pl.when(has_both)
        def _():
            kv_copy(1, 2, c, up).start()

        @pl.when(odd_and_down)
        def _():
            kv_copy(3, 2, c, pair).start()

    def relay_q(c):
        @pl.when(has_up)
        def _():
            q_copy(2, 0, c, down).wait_recv()

        @pl.when(has_both)
        def _():
            q_copy(1, 2, c, down).start()

        @pl.when(even_and_up)
        def _():
            q_copy(3, 2, c, pair).start()

    load_og.wait()
    for p in range(2):
        gather_start(0, p)

        @pl.when(has_down)
        def _():
            og_copy(2, 0, p, down).start()

        @pl.when(odd)
        def _():
            og_copy(3, 0, p, pair).start()

    for c in range(EARLY, heads):
        load_kv(c)

    for c in range(heads):
        pltpu.make_async_copy(
            q_hbm.at[:, cols(c, HDIM)], qs.at[c, 0], load_sem.at[3]
        ).start()

    tables = [
        pltpu.make_async_copy(table_hbm, table_ref, load_sem.at[5]),
        pltpu.make_async_copy(active_hbm, active_ref, load_sem.at[6]),
    ]
    for copy in tables:
        copy.start()

    def load_proj(t):
        part = pl.ds(t * 2 * HDIM, 2 * HDIM)
        return pltpu.make_async_copy(proj_hbm.at[part], proj.at[part], load_sem.at[4])

    def settle(ref, sem):
        return pltpu.make_async_copy(ref, ref, sem)

    pending = {
        "early": [settle(kv.at[:, pl.ds(0, EARLY), 0], load_sem.at[1])],
        "late": [settle(kv.at[:, pl.ds(EARLY, heads - EARLY), 0], load_sem.at[2])],
        "query": [settle(qs.at[:, 0], load_sem.at[3])],
        "proj": [settle(proj, load_sem.at[4])],
        "table": tables,
    }

    def ready(*names):
        for name in names:
            for copy in pending.pop(name, ()):
                copy.wait()

    here = {0: me >= 0, 1: has_near, 2: has_up, 3: even_or_up}
    reach = {1: has_far, 2: has_down, 3: odd_or_down}
    for k in range(1, SETS):

        @pl.when(jnp.logical_not(reach[k]))
        def _():
            @pl.loop(0, keyed)
            def _(c):
                for j in range(2):
                    kv[j, c, k] = jnp.zeros((rows, HDIM), BF16)

            for c in range(ASKED):
                part_in[c, k - 1] = jnp.full((3, rows), -FAR, F32)

        @pl.when(jnp.logical_not(here[k]))
        def _():
            @pl.loop(0, heads)
            def _(c):
                qs[c, k] = jnp.zeros((rows, HDIM), BF16)
                gs[c, k] = jnp.zeros((rows, HDIM), BF16)
                stat_in[c, k - 1] = jnp.full((2, rows), FAR, F32)

    for k, present in ((1, has_both), (2, has_down), (3, jnp.logical_or(odd, has_up))):

        @pl.when(jnp.logical_not(present))
        def _():
            for c in range(ASKED):
                back[c, k - 1] = jnp.zeros((HDIM, rows), BF16)

    def project(k, low, high):
        @pl.loop(low // 2, high // 2)
        def _(t):
            tile = proj[cols(t, 2 * HDIM), :]
            grad = dot(og[k], tile, ((1,), (1,))).astype(BF16)
            gs[2 * t, k] = grad[:, :HDIM]
            gs[2 * t + 1, k] = grad[:, HDIM:]

    key_index = lax.broadcasted_iota(jnp.int32, (rows, rows), 0)
    query_index = lax.broadcasted_iota(jnp.int32, (rows, rows), 1)

    def attend(c):
        ready("query", "table")
        for k in (1, 3):

            @pl.when(reach[k])
            def _():
                kv_copy(k, 0, c, me).wait_recv()

        query, grad = qs[c, 0], gs[c, 0]
        tops, totals, sums, exps, prob_grads = [], [], [], [], []
        for k in range(SETS):
            logits = dot(kv[0, c, k], query, ((1,), (1,))) * scale2
            if k == 0:
                logits = jnp.where(key_index <= query_index, logits, -FAR)
            prob_grads.append(dot(kv[1, c, k], grad, ((1,), (1,))))
            best = jnp.max(logits, axis=0, keepdims=True)
            exps.append(jnp.exp2(logits - best))
            totals.append(jnp.sum(exps[k], axis=0, keepdims=True))
            sums.append(jnp.sum(exps[k] * prob_grads[k], axis=0, keepdims=True))
            if k:
                usable = jnp.logical_and(
                    table_ref[k - 1, c] * active_ref[0, k - 1] > 0, me >= count // 2**k
                )
                best = best + jnp.where(usable, 0.0, -FAR).astype(F32)
            tops.append(best)
        top = functools.reduce(jnp.maximum, tops)
        shares = [jnp.exp2(x - top) for x in tops]
        total = sum(share * x for share, x in zip(shares, totals))
        inverse = 1.0 / total
        delta = sum(share * x for share, x in zip(shares, sums)) * inverse
        norm = top + jnp.log2(total)
        for k in range(1, SETS):
            hidden = jnp.where(active_ref[0, k - 1] > 0, 0.0, FAR).astype(F32)
            stat_out[c, k - 1] = jnp.concatenate([norm + hidden, delta], axis=0)

        probs = exps[0] * (shares[0] * inverse)
        dlogit = (probs * (prob_grads[0] - delta)).astype(BF16)
        terms = dot(kv[0, c, 0], dlogit, ((0,), (0,)))
        for k in range(1, SETS):
            part = (exps[k] * (prob_grads[k] - delta)).astype(BF16)
            terms = terms + dot(kv[0, c, k], part, ((0,), (0,))) * (shares[k] * inverse)
        own[0, c] = dot(dlogit, query, ((1,), (0,))) * scale
        own[1, c] = dot(probs.astype(BF16), grad, ((1,), (0,)))
        dq_ref[:, cols(c, HDIM)] = (terms * scale).T.astype(BF16)
        tell(c)

    def tell(c):
        group = group_of(c)
        if c + 1 < groups[group][1]:
            return

        for k, go, span in ((1, has_far, half), (2, has_down, quarter), (3, odd_or_down, eighth)):

            @pl.when(go)
            def _():
                stat_copy(k, group, me - span).start()

    heard = set()

    def hear(group):
        if group in heard:
            return

        heard.add(group)
        for k, span in ((1, half), (2, quarter), (3, eighth)):

            @pl.when(here[k])
            def _():
                stat_copy(k, group, me + span).wait_recv()

    asked_for = set()

    def meet(g):
        if g in asked_for:
            return

        asked_for.add(g)
        for k in (1, 3):

            @pl.when(here[k])
            def _():
                q_copy(k, 0, g, me).wait_recv()

    def collect(c):
        queries = qs[c, 1:].reshape(SECTIONS * rows, HDIM)
        grads = gs[c, 1:].reshape(SECTIONS * rows, HDIM)
        raw = dot(kv[0, c, 0], queries, ((1,), (1,))) * scale2
        prob_grad = dot(kv[1, c, 0], grads, ((1,), (1,)))
        weights, dlogits = [], []
        for k in range(1, SETS):
            part = slice((k - 1) * rows, k * rows)
            hidden = jnp.where(table_ref[k - 1, c] > 0, 0.0, FAR).astype(F32)
            probs = jnp.exp2(raw[:, part] - (stat_in[c, k - 1, 0:1] + hidden))
            weights.append(probs.astype(BF16))
            dlogits.append((probs * (prob_grad[:, part] - stat_in[c, k - 1, 1:2])).astype(BF16))
        key = dot(jnp.concatenate(dlogits, axis=1), queries, ((1,), (0,)))
        value = dot(jnp.concatenate(weights, axis=1), grads, ((1,), (0,)))
        dk_ref[:, cols(c, HDIM)] = (own[0, c] + key * scale).astype(BF16)
        dv_ref[:, cols(c, HDIM)] = (own[1, c] + value).astype(BF16)

    def finish(c):
        hear(group_of(c))
        meet(c // 2)
        collect(c)

    def arrive(k, p):
        @pl.when(here[k])
        def _():
            og_copy(k, 0, p, me).wait_recv()
            if k == 2:

                @pl.when(has_both)
                def _():
                    og_copy(1, 2, p, down).start()

                @pl.when(even)
                def _():
                    og_copy(3, 2, p, pair).start()

            gather_start(k, p)

    def hand_on(k):
        @pl.when(here[k])
        def _():
            gather_pass(k)

    def take(k, low=0, high=heads):
        ready("proj")

        @pl.when(here[k])
        def _():
            gather_end(k)
            project(k, low, high)

    def some(k):
        take(k, keyed, heads)

    def rest(k):
        @pl.when(here[k])
        def _():
            project(k, 0, keyed)

    def ask(first):
        ready("late", "table")
        for c in range(first, heads):
            if c % 2 == 0:
                meet(c // 2)

        for c in range(first, heads):
            ask_one(c)

        for k, span in ((1, half), (2, quarter), (3, eighth)):

            @pl.when(here[k])
            def _():
                part_copy(k, me + span).start()

    def ask_one(c):
        raw = dot(kv[0, c, 0], qs[c].reshape(SETS * rows, HDIM), ((1,), (1,))) * scale2
        prob_grad = dot(kv[1, c, 0], gs[c].reshape(SETS * rows, HDIM), ((1,), (1,)))
        for k in range(SETS):
            part = slice(k * rows, (k + 1) * rows)
            logits = raw[:, part]
            if k == 0:
                logits = jnp.where(key_index <= query_index, logits, -FAR)
            top = jnp.max(logits, axis=0, keepdims=True)
            exps = jnp.exp2(logits - top)
            total = jnp.sum(exps, axis=0, keepdims=True)
            weighted = jnp.sum(exps * prob_grad[:, part], axis=0, keepdims=True)
            if k == 0:
                part_own[c - keyed] = jnp.concatenate([top, total, weighted], axis=0)
            else:
                top = top + jnp.where(table_ref[k - 1, c] > 0, 0.0, -FAR).astype(F32)
                part_out[c - keyed, k - 1] = jnp.concatenate([top, total, weighted], axis=0)
    def combine(first):
        for k in range(1, SETS):

            @pl.when(reach[k])
            def _():
                part_copy(k, me).wait_recv()

        for c in range(first, heads):
            combine_one(c)

        tell(heads - 1)

    def combine_one(c):
        h = c - keyed
        tops, parts = [part_own[h, 0:1]], [(part_own[h, 1:2], part_own[h, 2:3])]
        for k in range(1, SETS):
            usable = jnp.logical_and(active_ref[0, k - 1] > 0, me >= count // 2**k)
            hidden = jnp.where(usable, 0.0, -FAR).astype(F32)
            tops.append(part_in[h, k - 1, 0:1] + hidden)
            sums = part_in[h, k - 1]
            parts.append((jnp.where(usable, sums[1:2], 0.0), jnp.where(usable, sums[2:3], 0.0)))
        top = functools.reduce(jnp.maximum, tops)
        shares = [jnp.exp2(x - top) for x in tops]
        total = sum(share * part[0] for share, part in zip(shares, parts))
        delta = sum(share * part[1] for share, part in zip(shares, parts)) / total
        norm = top + jnp.log2(total)
        stat_own[h] = jnp.concatenate([norm, delta], axis=0)
        for k in range(1, SETS):
            hidden = jnp.where(active_ref[0, k - 1] > 0, 0.0, FAR).astype(F32)
            stat_out[c, k - 1] = jnp.concatenate([norm + hidden, delta], axis=0)

    def answer(c):
        hear(group_of(c))
        h = c - keyed
        queries = qs[c].reshape(SETS * rows, HDIM)
        grads = gs[c].reshape(SETS * rows, HDIM)
        raw = dot(kv[0, c, 0], queries, ((1,), (1,))) * scale2
        prob_grad = dot(kv[1, c, 0], grads, ((1,), (1,)))
        weights, dlogits = [], []
        for k in range(SETS):
            part = slice(k * rows, (k + 1) * rows)
            logits = raw[:, part]
            if k == 0:
                logits = jnp.where(key_index <= query_index, logits, -FAR)
                norm, delta = stat_own[h, 0:1], stat_own[h, 1:2]
            else:
                hidden = jnp.where(table_ref[k - 1, c] > 0, 0.0, FAR).astype(F32)
                norm, delta = stat_in[c, k - 1, 0:1] + hidden, stat_in[c, k - 1, 1:2]
            probs = jnp.exp2(logits - norm)
            weights.append(probs.astype(BF16))
            dlogits.append((probs * (prob_grad[:, part] - delta)).astype(BF16))
        dlogit = jnp.concatenate(dlogits, axis=1)
        terms = dot(kv[0, c, 0], dlogit, ((0,), (0,))) * scale
        held[h] = terms[:, :rows]
        for k in range(1, SETS):
            term[h, k - 1] = terms[:, k * rows : (k + 1) * rows].astype(BF16)

        @pl.when(has_near)
        def _():
            term_copy(1, c, up).start()

        @pl.when(even_or_up)
        def _():
            term_copy(3, c, pair).start()

        dk_ref[:, cols(c, HDIM)] = (dot(dlogit, queries, ((1,), (0,))) * scale).astype(BF16)
        weight = jnp.concatenate(weights, axis=1)
        dv_ref[:, cols(c, HDIM)] = dot(weight, grads, ((1,), (0,))).astype(BF16)

    def merge(c):
        h = c - keyed

        @pl.when(has_both)
        def _():
            term_copy(1, c, me).wait_recv()

        @pl.when(jnp.logical_or(odd, has_up))
        def _():
            term_copy(3, c, me).wait_recv()

        @pl.when(has_up)
        def _():
            side = jnp.where(even, back[h, 2].astype(F32), 0.0)
            total = term[h, 1].astype(F32) + back[h, 0].astype(F32) + side
            term[h, 1] = total.astype(BF16)
            term_copy(2, c, up).start()

    def close(c):
        h = c - keyed

        @pl.when(has_down)
        def _():
            term_copy(2, c, me).wait_recv()

        side = jnp.where(odd, back[h, 2].astype(F32), 0.0)
        total = held[h] + back[h, 1].astype(F32) + side
        dq_ref[:, cols(c, HDIM)] = total.T.astype(BF16)

    plan = []
    for low, high, timed in (
        (
            0,
            keyed,
            (
                (send_kv, -35.51, 6.09),
                (relay_kv, -26.96, 13.35),
                (attend, 20.51, 7.47),
                (finish, 60.00, 14.65),
            ),
        ),
        (
            0,
            keyed // 2,
            (
                (side_q, -35.62, 5.18),
                (send_q, -20.83, 16.78),
                (relay_q, 16.85, 10.96),
            ),
        ),
        (
            keyed // 2,
            heads // 2,
            (
                (side_q, -45.00, 2.05),
                (send_q, -27.91, 178.66),
                (relay_q, -14.36, 42700.55),
            ),
        ),
        (
            keyed,
            heads,
            (
                (answer, 57.25, 0.32),
                (merge, 60.00, 25.48),
                (close, 119.40, 2041502.52),
            ),
        ),
    ):
        for action, start, step in timed:
            for c in range(low, high):
                plan.append((start + step * (c - low), functools.partial(action, c)))

    for due, action, *where in (
        (-27.93, arrive, 2, 0),
        (-24.44, arrive, 2, 1),
        (-20.90, hand_on, 0),
        (-16.89, arrive, 3, 0),
        (-10.96, hand_on, 2),
        (-5.70, arrive, 3, 1),
        (-1.75, take, 0),
        (3.61, take, 2),
        (10.57, arrive, 1, 0),
        (14.73, arrive, 1, 1),
        (17.89, hand_on, 3),
        (19.08, some, 3),
        (19.29, rest, 3),
        (21.27, hand_on, 1),
        (24.07, some, 1),
        (26.23, ask, keyed),
        (36.68, rest, 1),
        (37.92, combine, keyed),
    ):
        plan.append((due, functools.partial(action, *where)))

    for t in range(heads // 2):
        plan.append((-27.924 + t * 0.001, load_proj(t).start))

    plan.sort(key=lambda entry: entry[0])
    for _, action in plan:
        action()

    def drain(present, ref, sem):
        @pl.when(present)
        def _():
            settle(ref, sem).wait()

    always = me >= 0
    odd_or_up = jnp.logical_or(odd, has_up)
    drain(always, og.at[0, :, pl.ds(0, (lanes - 1) * width)], lane_send.at[0])
    for k, kv_sent, q_sent, term_sent in (
        (1, has_both, has_both, has_near),
        (2, has_up, has_down, has_up),
        (3, jnp.logical_or(even, has_down), odd_or_up, even_or_up),
    ):
        drain(here[k], og.at[k, :, pl.ds(0, (lanes - 1) * width)], lane_send.at[k])
        drain(q_sent, og.at[0, :, pl.ds(0, width)], og_send.at[k - 1])
        drain(q_sent, qs.at[:, k], q_send.at[k - 1])
        drain(kv_sent, kv.at[:, pl.ds(0, keyed), k], kv_send.at[k - 1])
        drain(reach[k], stat_out.at[:, k - 1], stat_send.at[k - 1])
        drain(here[k], part_out.at[:, k - 1], part_send.at[k - 1])
        drain(term_sent, term.at[:, k - 1], term_send.at[k - 1])


def publish_kernel(*refs):
    number = (len(refs) - 1) // 2
    copies = [
        pltpu.make_async_copy(refs[a], refs[number + a], refs[-1].at[a]) for a in range(number)
    ]
    for copy in copies:
        copy.start()
    for copy in copies:
        copy.wait()


def publish(arrays):
    number = len(arrays)
    held = [pltpu.with_memory_space_constraint(a, pltpu.VMEM) for a in arrays]
    return pl.pallas_call(
        publish_kernel,
        out_shape=[jax.ShapeDtypeStruct(a.shape, a.dtype) for a in arrays],
        in_specs=[pl.BlockSpec(memory_space=pltpu.VMEM)] * number,
        out_specs=[pl.BlockSpec(memory_space=pl.ANY)] * number,
        scratch_shapes=[pltpu.SemaphoreType.DMA((number,))],
        compiler_params=pltpu.CompilerParams(vmem_limit_bytes=2**20),
    )(*held)


def body(count, lanes, queries, key_rows, value_rows, out_grad, out_proj, table, active):
    rows, columns = queries.shape
    heads = columns // HDIM
    vmem = pl.BlockSpec(memory_space=pltpu.VMEM)
    hbm = pl.BlockSpec(memory_space=pl.ANY)
    dma = pltpu.SemaphoreType.DMA
    grads = pl.pallas_call(
        functools.partial(kernel, count, lanes),
        out_shape=[pltpu.VMEM((rows, columns), BF16)] * 3,
        in_specs=[hbm] * 7,
        out_specs=[vmem] * 3,
        scratch_shapes=[
            pltpu.VMEM((2, heads, SETS, rows, HDIM), BF16),
            pltpu.VMEM((heads, SETS, rows, HDIM), BF16),
            pltpu.VMEM((heads, SETS, rows, HDIM), BF16),
            pltpu.VMEM((SETS, rows, out_proj.shape[1]), BF16),
            pltpu.VMEM(out_proj.shape, BF16),
            pltpu.VMEM((2, heads, rows, HDIM), F32),
            pltpu.VMEM((heads, SECTIONS, 2, rows), F32),
            pltpu.VMEM((heads, SECTIONS, 2, rows), F32),
            pltpu.VMEM((ASKED, 3, rows), F32),
            pltpu.VMEM((ASKED, SECTIONS, 3, rows), F32),
            pltpu.VMEM((ASKED, SECTIONS, 3, rows), F32),
            pltpu.VMEM((ASKED, 2, rows), F32),
            pltpu.VMEM((ASKED, HDIM, rows), F32),
            pltpu.VMEM((ASKED, SECTIONS, HDIM, rows), BF16),
            pltpu.VMEM((ASKED, SECTIONS, HDIM, rows), BF16),
            pltpu.SMEM((SECTIONS, heads), jnp.int32),
            pltpu.SMEM((1, SECTIONS), jnp.int32),
            dma((7,)),
            dma((SECTIONS,)),
            dma((SECTIONS, heads - ASKED)),
            dma((SECTIONS,)),
            dma((SECTIONS, heads // 2)),
            dma((SECTIONS,)),
            dma((SECTIONS, 2)),
            dma((SETS,)),
            dma((SETS, 2, max(1, lanes // 2 - 1))),
            dma((SETS,)),
            dma((SECTIONS,)),
            dma((SECTIONS, 4)),
            dma((SECTIONS,)),
            dma((SECTIONS,)),
            dma((SECTIONS,)),
            dma((SECTIONS, ASKED)),
        ],
        compiler_params=pltpu.CompilerParams(
            collective_id=0, has_side_effects=True, vmem_limit_bytes=60 * 2**20
        ),
    )(queries, key_rows, value_rows, out_grad, out_proj, table.T, active)
    return tuple(publish(grads))


def solution(mesh):
    return jax.shard_map(
        functools.partial(body, mesh.shape["seq"], mesh.shape["head"]),
        mesh=mesh,
        in_specs=(
            P("seq", "head"),
            P("seq", "head"),
            P("seq", "head"),
            P("seq", "head"),
            P("head", None),
            P("head", None),
            P("seq", None),
        ),
        out_specs=(P("seq", "head"), P("seq", "head"), P("seq", "head")),
        check_vma=False,
    )
```

```python
import functools
import math

import jax
import jax.numpy as jnp
from jax import lax
from jax.experimental import pallas as pl
from jax.experimental.pallas import tpu as pltpu
from jax.sharding import PartitionSpec as P

HDIM = 128
SECTIONS = 3
SETS = SECTIONS + 1
ASKED = 2
EARLY = 2
FAR = 1e30
MESH = pl.DeviceIdType.MESH
BF16 = jnp.bfloat16
F32 = jnp.float32


def dot(a, b, dims):
    return lax.dot_general(a, b, (dims, ((), ())), preferred_element_type=F32)


def kernel(
    count,
    lanes,
    q_hbm,
    k_hbm,
    v_hbm,
    og_hbm,
    proj_hbm,
    table_hbm,
    active_hbm,
    dq_ref,
    dk_ref,
    dv_ref,
    kv,
    qs,
    gs,
    og,
    proj,
    own,
    stat_out,
    stat_in,
    part_own,
    part_out,
    part_in,
    stat_own,
    held,
    term,
    back,
    table_ref,
    active_ref,
    load_sem,
    kv_send,
    kv_recv,
    q_send,
    q_recv,
    og_send,
    og_recv,
    lane_send,
    peer_recv,
    twin_recv,
    stat_send,
    stat_recv,
    part_send,
    part_recv,
    term_send,
    term_recv,
):
    _, heads, _, rows, _ = kv.shape
    width = og.shape[2] // lanes
    piece = rows // 2
    keyed = heads - ASKED
    scale = 1.0 / math.sqrt(HDIM)
    scale2 = scale / math.log(2.0)
    half, quarter, eighth = count // 2, count // 4, count // 8
    me = lax.axis_index("seq")
    lane = lax.axis_index("head")
    odd = (me // eighth) % 2 == 1
    even = jnp.logical_not(odd)
    up, down = me + quarter, me - quarter
    pair = jnp.where(odd, me - eighth, me + eighth)
    other = jnp.where(odd, me + eighth, me - eighth)
    has_up, has_down = me < count - quarter, me >= quarter
    has_far, has_near = me >= half, me < count - half
    has_both = jnp.logical_and(has_up, has_down)
    odd_or_down = jnp.logical_or(odd, has_down)
    even_or_up = jnp.logical_or(even, has_up)
    odd_and_down = jnp.logical_and(odd, has_down)
    even_and_up = jnp.logical_and(even, has_up)
    has_other = jnp.where(odd, has_up, has_down)
    twin = jnp.where(lane % 2 == 1, lane - 1, lane + 1)
    peers = [lax.rem(lane + 2 * j, lanes) for j in range(1, lanes // 2)]

    def cols(c, size):
        return pl.ds(pl.multiple_of(c * size, size), size)

    def remote(src, dst, send, recv, axis, target):
        return pltpu.make_async_remote_copy(
            src_ref=src,
            dst_ref=dst,
            send_sem=send,
            recv_sem=recv,
            device_id={axis: target},
            device_id_type=MESH,
        )

    def kv_copy(k, source, c, target):
        return remote(
            kv.at[:, c, source],
            kv.at[:, c, k],
            kv_send.at[k - 1],
            kv_recv.at[k - 1, c],
            "seq",
            target,
        )

    def q_copy(k, source, g, target):
        duo = pl.ds(2 * g, 2)
        return remote(
            qs.at[duo, source],
            qs.at[duo, k],
            q_send.at[k - 1],
            q_recv.at[k - 1, g],
            "seq",
            target,
        )

    def og_copy(k, source, p, target):
        part = pl.ds(p * piece, piece)
        return remote(
            og.at[source, part, cols(lane, width)],
            og.at[k, part, cols(lane, width)],
            og_send.at[k - 1],
            og_recv.at[k - 1, p],
            "seq",
            target,
        )

    def peer_copy(k, j, shard, p, target):
        part = og.at[k, pl.ds(p * piece, piece), cols(shard, width)]
        return remote(part, part, lane_send.at[k], peer_recv.at[k, p, j], "head", target)

    def twin_copy(k, shard, p):
        part = og.at[k, pl.ds(p * piece, piece), cols(shard, width)]
        return remote(part, part, lane_send.at[k], twin_recv.at[k], "head", twin)

    def part_copy(k, target):
        return remote(
            part_out.at[:, k - 1],
            part_in.at[:, k - 1],
            part_send.at[k - 1],
            part_recv.at[k - 1],
            "seq",
            target,
        )

    def term_copy(k, c, target):
        return remote(
            term.at[c - keyed, k - 1],
            back.at[c - keyed, k - 1],
            term_send.at[k - 1],
            term_recv.at[k - 1, c - keyed],
            "seq",
            target,
        )

    groups = [(0, keyed - 2), (keyed - 2, keyed - 1), (keyed - 1, keyed), (keyed, heads)]

    def group_of(c):
        return [low <= c < high for low, high in groups].index(True)

    def stat_copy(k, group, target):
        low, high = groups[group]
        some_heads = pl.ds(low, high - low)
        return remote(
            stat_out.at[some_heads, k - 1],
            stat_in.at[some_heads, k - 1],
            stat_send.at[k - 1],
            stat_recv.at[k - 1, group],
            "seq",
            target,
        )

    barrier = pltpu.get_barrier_semaphore()
    arrivals = jnp.int32(2 + len(peers))
    for peer in [twin] + peers:
        pl.semaphore_signal(barrier, inc=1, device_id={"head": peer}, device_id_type=MESH)
    pl.semaphore_signal(barrier, inc=1, device_id={"seq": pair}, device_id_type=MESH)
    for present, target in (
        (has_up, up),
        (has_down, down),
        (has_far, me - half),
        (has_near, me + half),
        (has_other, other),
    ):
        arrivals = arrivals + present.astype(jnp.int32)

        @pl.when(present)
        def _():
            pl.semaphore_signal(barrier, inc=1, device_id={"seq": target}, device_id_type=MESH)

    load_og = pltpu.make_async_copy(og_hbm, og.at[0, :, cols(lane, width)], load_sem.at[0])

    def load_kv(c):
        for j, source in enumerate((k_hbm, v_hbm)):
            pltpu.make_async_copy(
                source.at[:, cols(c, HDIM)],
                kv.at[j, c, 0],
                load_sem.at[1 if c < EARLY else 2],
            ).start()

    load_og.start()
    for c in range(EARLY):
        load_kv(c)

    pl.semaphore_wait(barrier, arrivals)

    def gather_start(k, p):
        for j, peer in enumerate(peers):
            peer_copy(k, j, lane, p, peer).start()
        twin_copy(k, lane, p).start()

    def gather_pass(k):
        for p in range(2):
            for j in range(len(peers)):
                shard = lax.rem(lane + lanes - 2 * (j + 1), lanes)
                peer_copy(k, j, shard, p, lane).wait_recv()
                twin_copy(k, shard, p).start()

    def gather_end(k):
        settle(og.at[k, :, pl.ds(0, lanes // 2 * width)], twin_recv.at[k]).wait()

    def send_kv(c):
        ready("early" if c < EARLY else "late")

        @pl.when(has_up)
        def _():
            kv_copy(2, 0, c, up).start()

        @pl.when(even)
        def _():
            kv_copy(3, 0, c, pair).start()

    def send_q(c):
        ready("query")

        @pl.when(has_down)
        def _():
            q_copy(2, 0, c, down).start()

    def side_q(c):
        ready("query")

        @pl.when(odd)
        def _():
            q_copy(3, 0, c, pair).start()

    def relay_kv(c):
        @pl.when(has_down)
        def _():
            kv_copy(2, 0, c, up).wait_recv()

        @pl.when(has_both)
        def _():
            kv_copy(1, 2, c, up).start()

        @pl.when(odd_and_down)
        def _():
            kv_copy(3, 2, c, pair).start()

    def relay_q(c):
        @pl.when(has_up)
        def _():
            q_copy(2, 0, c, down).wait_recv()

        @pl.when(has_both)
        def _():
            q_copy(1, 2, c, down).start()

        @pl.when(even_and_up)
        def _():
            q_copy(3, 2, c, pair).start()

    tables = [
        pltpu.make_async_copy(table_hbm, table_ref, load_sem.at[5]),
        pltpu.make_async_copy(active_hbm, active_ref, load_sem.at[6]),
    ]
    def load_proj(t):
        part = pl.ds(t * 2 * HDIM, 2 * HDIM)
        return pltpu.make_async_copy(proj_hbm.at[part], proj.at[part], load_sem.at[4])

    def settle(ref, sem):
        return pltpu.make_async_copy(ref, ref, sem)

    pending = {
        "early": [settle(kv.at[:, pl.ds(0, EARLY), 0], load_sem.at[1])],
        "late": [settle(kv.at[:, pl.ds(EARLY, heads - EARLY), 0], load_sem.at[2])],
        "query": [settle(qs.at[:, 0], load_sem.at[3])],
        "proj": [settle(proj, load_sem.at[4])],
        "table": tables,
    }

    def ready(*names):
        for name in names:
            for copy in pending.pop(name, ()):
                copy.wait()

    here = {0: me >= 0, 1: has_near, 2: has_up, 3: even_or_up}
    reach = {1: has_far, 2: has_down, 3: odd_or_down}
    def fetch():
        for c in range(EARLY, heads):
            load_kv(c)

        for c in range(heads):
            pltpu.make_async_copy(
                q_hbm.at[:, cols(c, HDIM)], qs.at[c, 0], load_sem.at[3]
            ).start()

        for copy in tables:
            copy.start()

    def clear():
        for k in range(1, SETS):

            @pl.when(jnp.logical_not(reach[k]))
            def _():
                @pl.loop(0, keyed)
                def _(c):
                    for j in range(2):
                        kv[j, c, k] = jnp.zeros((rows, HDIM), BF16)

                for c in range(ASKED):
                    part_in[c, k - 1] = jnp.full((3, rows), -FAR, F32)

            @pl.when(jnp.logical_not(here[k]))
            def _():
                @pl.loop(0, heads)
                def _(c):
                    qs[c, k] = jnp.zeros((rows, HDIM), BF16)
                    gs[c, k] = jnp.zeros((rows, HDIM), BF16)
                    stat_in[c, k - 1] = jnp.full((2, rows), FAR, F32)

        for k, present in ((1, has_both), (2, has_down), (3, jnp.logical_or(odd, has_up))):

            @pl.when(jnp.logical_not(present))
            def _():
                for c in range(ASKED):
                    back[c, k - 1] = jnp.zeros((HDIM, rows), BF16)

    load_og.wait()
    for p in range(2):
        gather_start(0, p)

        @pl.when(has_down)
        def _():
            og_copy(2, 0, p, down).start()

        @pl.when(odd)
        def _():
            og_copy(3, 0, p, pair).start()

    for c in range(EARLY):
        send_kv(c)

    fetch()

    def project(k, low, high):
        @pl.loop(low // 2, high // 2)
        def _(t):
            tile = proj[cols(t, 2 * HDIM), :]
            grad = dot(og[k], tile, ((1,), (1,))).astype(BF16)
            gs[2 * t, k] = grad[:, :HDIM]
            gs[2 * t + 1, k] = grad[:, HDIM:]

    key_index = lax.broadcasted_iota(jnp.int32, (rows, rows), 0)
    query_index = lax.broadcasted_iota(jnp.int32, (rows, rows), 1)

    def attend(c):
        ready("query", "table")
        for k in (1, 3):

            @pl.when(reach[k])
            def _():
                kv_copy(k, 0, c, me).wait_recv()

        query, grad = qs[c, 0], gs[c, 0]
        tops, totals, sums, exps, prob_grads = [], [], [], [], []
        for k in range(SETS):
            logits = dot(kv[0, c, k], query, ((1,), (1,))) * scale2
            if k == 0:
                logits = jnp.where(key_index <= query_index, logits, -FAR)
            prob_grads.append(dot(kv[1, c, k], grad, ((1,), (1,))))
            best = jnp.max(logits, axis=0, keepdims=True)
            exps.append(jnp.exp2(logits - best))
            totals.append(jnp.sum(exps[k], axis=0, keepdims=True))
            sums.append(jnp.sum(exps[k] * prob_grads[k], axis=0, keepdims=True))
            if k:
                usable = jnp.logical_and(
                    table_ref[k - 1, c] * active_ref[0, k - 1] > 0, me >= count // 2**k
                )
                best = best + jnp.where(usable, 0.0, -FAR).astype(F32)
            tops.append(best)
        top = functools.reduce(jnp.maximum, tops)
        shares = [jnp.exp2(x - top) for x in tops]
        total = sum(share * x for share, x in zip(shares, totals))
        inverse = 1.0 / total
        delta = sum(share * x for share, x in zip(shares, sums)) * inverse
        norm = top + jnp.log2(total)
        for k in range(1, SETS):
            hidden = jnp.where(active_ref[0, k - 1] > 0, 0.0, FAR).astype(F32)
            stat_out[c, k - 1] = jnp.concatenate([norm + hidden, delta], axis=0)

        probs = exps[0] * (shares[0] * inverse)
        dlogit = (probs * (prob_grads[0] - delta)).astype(BF16)
        terms = dot(kv[0, c, 0], dlogit, ((0,), (0,)))
        for k in range(1, SETS):
            part = (exps[k] * (prob_grads[k] - delta)).astype(BF16)
            terms = terms + dot(kv[0, c, k], part, ((0,), (0,))) * (shares[k] * inverse)
        own[0, c] = dot(dlogit, query, ((1,), (0,))) * scale
        own[1, c] = dot(probs.astype(BF16), grad, ((1,), (0,)))
        dq_ref[:, cols(c, HDIM)] = (terms * scale).T.astype(BF16)
        tell(c)

    def tell(c):
        group = group_of(c)
        if c + 1 < groups[group][1]:
            return

        for k, go, span in ((1, has_far, half), (2, has_down, quarter), (3, odd_or_down, eighth)):

            @pl.when(go)
            def _():
                stat_copy(k, group, me - span).start()

    heard = set()

    def hear(group):
        if group in heard:
            return

        heard.add(group)
        for k, span in ((1, half), (2, quarter), (3, eighth)):

            @pl.when(here[k])
            def _():
                stat_copy(k, group, me + span).wait_recv()

    asked_for = set()

    def meet(g):
        if g in asked_for:
            return

        asked_for.add(g)
        for k in (1, 3):

            @pl.when(here[k])
            def _():
                q_copy(k, 0, g, me).wait_recv()

    def collect(c):
        queries = qs[c, 1:].reshape(SECTIONS * rows, HDIM)
        grads = gs[c, 1:].reshape(SECTIONS * rows, HDIM)
        raw = dot(kv[0, c, 0], queries, ((1,), (1,))) * scale2
        prob_grad = dot(kv[1, c, 0], grads, ((1,), (1,)))
        weights, dlogits = [], []
        for k in range(1, SETS):
            part = slice((k - 1) * rows, k * rows)
            hidden = jnp.where(table_ref[k - 1, c] > 0, 0.0, FAR).astype(F32)
            probs = jnp.exp2(raw[:, part] - (stat_in[c, k - 1, 0:1] + hidden))
            weights.append(probs.astype(BF16))
            dlogits.append((probs * (prob_grad[:, part] - stat_in[c, k - 1, 1:2])).astype(BF16))
        key = dot(jnp.concatenate(dlogits, axis=1), queries, ((1,), (0,)))
        value = dot(jnp.concatenate(weights, axis=1), grads, ((1,), (0,)))
        dk_ref[:, cols(c, HDIM)] = (own[0, c] + key * scale).astype(BF16)
        dv_ref[:, cols(c, HDIM)] = (own[1, c] + value).astype(BF16)

    def finish(c):
        hear(group_of(c))
        meet(c // 2)
        collect(c)

    def arrive(k, p):
        @pl.when(here[k])
        def _():
            og_copy(k, 0, p, me).wait_recv()
            if k == 2:

                @pl.when(has_both)
                def _():
                    og_copy(1, 2, p, down).start()

                @pl.when(even)
                def _():
                    og_copy(3, 2, p, pair).start()

            gather_start(k, p)

    def hand_on(k):
        @pl.when(here[k])
        def _():
            gather_pass(k)

    def take(k, low=0, high=heads):
        ready("proj")

        @pl.when(here[k])
        def _():
            gather_end(k)
            project(k, low, high)

    def some(k):
        take(k, keyed, heads)

    def rest(k):
        @pl.when(here[k])
        def _():
            project(k, 0, keyed)

    def ask(first):
        ready("late", "table")
        for c in range(first, heads):
            if c % 2 == 0:
                meet(c // 2)

        for c in range(first, heads):
            ask_one(c)

        for k, span in ((1, half), (2, quarter), (3, eighth)):

            @pl.when(here[k])
            def _():
                part_copy(k, me + span).start()

    def ask_one(c):
        raw = dot(kv[0, c, 0], qs[c].reshape(SETS * rows, HDIM), ((1,), (1,))) * scale2
        prob_grad = dot(kv[1, c, 0], gs[c].reshape(SETS * rows, HDIM), ((1,), (1,)))
        for k in range(SETS):
            part = slice(k * rows, (k + 1) * rows)
            logits = raw[:, part]
            if k == 0:
                logits = jnp.where(key_index <= query_index, logits, -FAR)
            top = jnp.max(logits, axis=0, keepdims=True)
            exps = jnp.exp2(logits - top)
            total = jnp.sum(exps, axis=0, keepdims=True)
            weighted = jnp.sum(exps * prob_grad[:, part], axis=0, keepdims=True)
            if k == 0:
                part_own[c - keyed] = jnp.concatenate([top, total, weighted], axis=0)
            else:
                top = top + jnp.where(table_ref[k - 1, c] > 0, 0.0, -FAR).astype(F32)
                part_out[c - keyed, k - 1] = jnp.concatenate([top, total, weighted], axis=0)
    def combine(first):
        for k in range(1, SETS):

            @pl.when(reach[k])
            def _():
                part_copy(k, me).wait_recv()

        for c in range(first, heads):
            combine_one(c)

        tell(heads - 1)

    def combine_one(c):
        h = c - keyed
        tops, parts = [part_own[h, 0:1]], [(part_own[h, 1:2], part_own[h, 2:3])]
        for k in range(1, SETS):
            usable = jnp.logical_and(active_ref[0, k - 1] > 0, me >= count // 2**k)
            hidden = jnp.where(usable, 0.0, -FAR).astype(F32)
            tops.append(part_in[h, k - 1, 0:1] + hidden)
            sums = part_in[h, k - 1]
            parts.append((jnp.where(usable, sums[1:2], 0.0), jnp.where(usable, sums[2:3], 0.0)))
        top = functools.reduce(jnp.maximum, tops)
        shares = [jnp.exp2(x - top) for x in tops]
        total = sum(share * part[0] for share, part in zip(shares, parts))
        delta = sum(share * part[1] for share, part in zip(shares, parts)) / total
        norm = top + jnp.log2(total)
        stat_own[h] = jnp.concatenate([norm, delta], axis=0)
        for k in range(1, SETS):
            hidden = jnp.where(active_ref[0, k - 1] > 0, 0.0, FAR).astype(F32)
            stat_out[c, k - 1] = jnp.concatenate([norm + hidden, delta], axis=0)

    def answer(c):
        hear(group_of(c))
        h = c - keyed
        queries = qs[c].reshape(SETS * rows, HDIM)
        grads = gs[c].reshape(SETS * rows, HDIM)
        raw = dot(kv[0, c, 0], queries, ((1,), (1,))) * scale2
        prob_grad = dot(kv[1, c, 0], grads, ((1,), (1,)))
        weights, dlogits = [], []
        for k in range(SETS):
            part = slice(k * rows, (k + 1) * rows)
            logits = raw[:, part]
            if k == 0:
                logits = jnp.where(key_index <= query_index, logits, -FAR)
                norm, delta = stat_own[h, 0:1], stat_own[h, 1:2]
            else:
                hidden = jnp.where(table_ref[k - 1, c] > 0, 0.0, FAR).astype(F32)
                norm, delta = stat_in[c, k - 1, 0:1] + hidden, stat_in[c, k - 1, 1:2]
            probs = jnp.exp2(logits - norm)
            weights.append(probs.astype(BF16))
            dlogits.append((probs * (prob_grad[:, part] - delta)).astype(BF16))
        dlogit = jnp.concatenate(dlogits, axis=1)
        terms = dot(kv[0, c, 0], dlogit, ((0,), (0,))) * scale
        held[h] = terms[:, :rows]
        for k in range(1, SETS):
            term[h, k - 1] = terms[:, k * rows : (k + 1) * rows].astype(BF16)

        @pl.when(has_near)
        def _():
            term_copy(1, c, up).start()

        @pl.when(even_or_up)
        def _():
            term_copy(3, c, pair).start()

        dk_ref[:, cols(c, HDIM)] = (dot(dlogit, queries, ((1,), (0,))) * scale).astype(BF16)
        weight = jnp.concatenate(weights, axis=1)
        dv_ref[:, cols(c, HDIM)] = dot(weight, grads, ((1,), (0,))).astype(BF16)

    def merge(c):
        h = c - keyed

        @pl.when(has_both)
        def _():
            term_copy(1, c, me).wait_recv()

        @pl.when(jnp.logical_or(odd, has_up))
        def _():
            term_copy(3, c, me).wait_recv()

        @pl.when(has_up)
        def _():
            side = jnp.where(even, back[h, 2].astype(F32), 0.0)
            total = term[h, 1].astype(F32) + back[h, 0].astype(F32) + side
            term[h, 1] = total.astype(BF16)
            term_copy(2, c, up).start()

    def close(c):
        h = c - keyed

        @pl.when(has_down)
        def _():
            term_copy(2, c, me).wait_recv()

        side = jnp.where(odd, back[h, 2].astype(F32), 0.0)
        total = held[h] + back[h, 1].astype(F32) + side
        dq_ref[:, cols(c, HDIM)] = total.T.astype(BF16)

    plan = []
    for low, high, timed in (
        (EARLY, keyed, ((send_kv, -23.33, 6.09),)),
        (
            0,
            keyed,
            (
                (relay_kv, -26.96, 13.35),
                (attend, 20.51, 7.47),
                (finish, 60.00, 14.65),
            ),
        ),
        (
            0,
            keyed // 2,
            (
                (side_q, -35.62, 5.18),
                (send_q, -20.83, 16.78),
                (relay_q, 16.85, 10.96),
            ),
        ),
        (
            keyed // 2,
            heads // 2,
            (
                (side_q, -45.00, 2.05),
                (send_q, -27.91, 178.66),
                (relay_q, -14.36, 42700.55),
            ),
        ),
        (
            keyed,
            heads,
            (
                (answer, 57.25, 0.32),
                (merge, 60.00, 25.48),
                (close, 119.40, 2041502.52),
            ),
        ),
    ):
        for action, start, step in timed:
            for c in range(low, high):
                plan.append((start + step * (c - low), functools.partial(action, c)))

    for due, action, *where in (
        (-27.93, arrive, 2, 0),
        (-24.44, arrive, 2, 1),
        (-20.90, hand_on, 0),
        (-16.89, arrive, 3, 0),
        (-10.96, hand_on, 2),
        (-5.70, arrive, 3, 1),
        (-1.75, take, 0),
        (3.61, take, 2),
        (10.57, arrive, 1, 0),
        (14.73, arrive, 1, 1),
        (17.89, hand_on, 3),
        (19.08, some, 3),
        (19.29, rest, 3),
        (21.27, hand_on, 1),
        (24.07, some, 1),
        (26.23, ask, keyed),
        (36.68, rest, 1),
        (37.92, combine, keyed),
    ):
        plan.append((due, functools.partial(action, *where)))

    for t in range(heads // 2):
        plan.append((-27.924 + t * 0.001, load_proj(t).start))

    plan.append((-27.918, clear))
    plan.sort(key=lambda entry: entry[0])
    for _, action in plan:
        action()

    def drain(present, ref, sem):
        @pl.when(present)
        def _():
            settle(ref, sem).wait()

    always = me >= 0
    odd_or_up = jnp.logical_or(odd, has_up)
    drain(always, og.at[0, :, pl.ds(0, (lanes - 1) * width)], lane_send.at[0])
    for k, kv_sent, q_sent, term_sent in (
        (1, has_both, has_both, has_near),
        (2, has_up, has_down, has_up),
        (3, jnp.logical_or(even, has_down), odd_or_up, even_or_up),
    ):
        drain(here[k], og.at[k, :, pl.ds(0, (lanes - 1) * width)], lane_send.at[k])
        drain(q_sent, og.at[0, :, pl.ds(0, width)], og_send.at[k - 1])
        drain(q_sent, qs.at[:, k], q_send.at[k - 1])
        drain(kv_sent, kv.at[:, pl.ds(0, keyed), k], kv_send.at[k - 1])
        drain(reach[k], stat_out.at[:, k - 1], stat_send.at[k - 1])
        drain(here[k], part_out.at[:, k - 1], part_send.at[k - 1])
        drain(term_sent, term.at[:, k - 1], term_send.at[k - 1])


def publish_kernel(*refs):
    number = (len(refs) - 1) // 2
    copies = [
        pltpu.make_async_copy(refs[a], refs[number + a], refs[-1].at[a]) for a in range(number)
    ]
    for copy in copies:
        copy.start()
    for copy in copies:
        copy.wait()


def publish(arrays):
    number = len(arrays)
    held = [pltpu.with_memory_space_constraint(a, pltpu.VMEM) for a in arrays]
    return pl.pallas_call(
        publish_kernel,
        out_shape=[jax.ShapeDtypeStruct(a.shape, a.dtype) for a in arrays],
        in_specs=[pl.BlockSpec(memory_space=pltpu.VMEM)] * number,
        out_specs=[pl.BlockSpec(memory_space=pl.ANY)] * number,
        scratch_shapes=[pltpu.SemaphoreType.DMA((number,))],
        compiler_params=pltpu.CompilerParams(vmem_limit_bytes=2**20),
    )(*held)


def body(count, lanes, queries, key_rows, value_rows, out_grad, out_proj, table, active):
    rows, columns = queries.shape
    heads = columns // HDIM
    vmem = pl.BlockSpec(memory_space=pltpu.VMEM)
    hbm = pl.BlockSpec(memory_space=pl.ANY)
    dma = pltpu.SemaphoreType.DMA
    grads = pl.pallas_call(
        functools.partial(kernel, count, lanes),
        out_shape=[pltpu.VMEM((rows, columns), BF16)] * 3,
        in_specs=[hbm] * 7,
        out_specs=[vmem] * 3,
        scratch_shapes=[
            pltpu.VMEM((2, heads, SETS, rows, HDIM), BF16),
            pltpu.VMEM((heads, SETS, rows, HDIM), BF16),
            pltpu.VMEM((heads, SETS, rows, HDIM), BF16),
            pltpu.VMEM((SETS, rows, out_proj.shape[1]), BF16),
            pltpu.VMEM(out_proj.shape, BF16),
            pltpu.VMEM((2, heads, rows, HDIM), F32),
            pltpu.VMEM((heads, SECTIONS, 2, rows), F32),
            pltpu.VMEM((heads, SECTIONS, 2, rows), F32),
            pltpu.VMEM((ASKED, 3, rows), F32),
            pltpu.VMEM((ASKED, SECTIONS, 3, rows), F32),
            pltpu.VMEM((ASKED, SECTIONS, 3, rows), F32),
            pltpu.VMEM((ASKED, 2, rows), F32),
            pltpu.VMEM((ASKED, HDIM, rows), F32),
            pltpu.VMEM((ASKED, SECTIONS, HDIM, rows), BF16),
            pltpu.VMEM((ASKED, SECTIONS, HDIM, rows), BF16),
            pltpu.SMEM((SECTIONS, heads), jnp.int32),
            pltpu.SMEM((1, SECTIONS), jnp.int32),
            dma((7,)),
            dma((SECTIONS,)),
            dma((SECTIONS, heads - ASKED)),
            dma((SECTIONS,)),
            dma((SECTIONS, heads // 2)),
            dma((SECTIONS,)),
            dma((SECTIONS, 2)),
            dma((SETS,)),
            dma((SETS, 2, max(1, lanes // 2 - 1))),
            dma((SETS,)),
            dma((SECTIONS,)),
            dma((SECTIONS, 4)),
            dma((SECTIONS,)),
            dma((SECTIONS,)),
            dma((SECTIONS,)),
            dma((SECTIONS, ASKED)),
        ],
        compiler_params=pltpu.CompilerParams(
            collective_id=0, has_side_effects=True, vmem_limit_bytes=60 * 2**20
        ),
    )(queries, key_rows, value_rows, out_grad, out_proj, table.T, active)
    return tuple(publish(grads))


def solution(mesh):
    return jax.shard_map(
        functools.partial(body, mesh.shape["seq"], mesh.shape["head"]),
        mesh=mesh,
        in_specs=(
            P("seq", "head"),
            P("seq", "head"),
            P("seq", "head"),
            P("seq", "head"),
            P("head", None),
            P("head", None),
            P("seq", None),
        ),
        out_specs=(P("seq", "head"), P("seq", "head"), P("seq", "head")),
        check_vma=False,
    )
```

```python
import functools
import math

import jax
import jax.numpy as jnp
from jax import lax
from jax.experimental import pallas as pl
from jax.experimental.pallas import tpu as pltpu
from jax.sharding import PartitionSpec as P

HDIM = 128
SECTIONS = 3
SETS = SECTIONS + 1
ASKED = 2
EARLY = 2
FAR = 1e30
MESH = pl.DeviceIdType.MESH
BF16 = jnp.bfloat16
F32 = jnp.float32


def dot(a, b, dims):
    return lax.dot_general(a, b, (dims, ((), ())), preferred_element_type=F32)


def kernel(
    count,
    lanes,
    q_hbm,
    k_hbm,
    v_hbm,
    og_hbm,
    proj_hbm,
    table_hbm,
    active_hbm,
    dq_ref,
    dk_ref,
    dv_ref,
    kv,
    qs,
    gs,
    og,
    proj,
    own,
    stat_out,
    stat_in,
    part_own,
    part_out,
    part_in,
    stat_own,
    held,
    term,
    back,
    table_ref,
    active_ref,
    load_sem,
    kv_send,
    kv_recv,
    q_send,
    q_recv,
    og_send,
    og_recv,
    lane_send,
    peer_recv,
    twin_recv,
    stat_send,
    stat_recv,
    part_send,
    part_recv,
    term_send,
    term_recv,
):
    _, heads, _, rows, _ = kv.shape
    width = og.shape[2] // lanes
    piece = rows // 2
    keyed = heads - ASKED
    scale = 1.0 / math.sqrt(HDIM)
    scale2 = scale / math.log(2.0)
    half, quarter, eighth = count // 2, count // 4, count // 8
    me = lax.axis_index("seq")
    lane = lax.axis_index("head")
    odd = (me // eighth) % 2 == 1
    even = jnp.logical_not(odd)
    up, down = me + quarter, me - quarter
    pair = jnp.where(odd, me - eighth, me + eighth)
    other = jnp.where(odd, me + eighth, me - eighth)
    has_up, has_down = me < count - quarter, me >= quarter
    has_far, has_near = me >= half, me < count - half
    has_both = jnp.logical_and(has_up, has_down)
    odd_or_down = jnp.logical_or(odd, has_down)
    even_or_up = jnp.logical_or(even, has_up)
    odd_and_down = jnp.logical_and(odd, has_down)
    even_and_up = jnp.logical_and(even, has_up)
    has_other = jnp.where(odd, has_up, has_down)
    twin = jnp.where(lane % 2 == 1, lane - 1, lane + 1)
    peers = [lax.rem(lane + 2 * j, lanes) for j in range(1, lanes // 2)]

    def cols(c, size):
        return pl.ds(pl.multiple_of(c * size, size), size)

    def remote(src, dst, send, recv, axis, target):
        return pltpu.make_async_remote_copy(
            src_ref=src,
            dst_ref=dst,
            send_sem=send,
            recv_sem=recv,
            device_id={axis: target},
            device_id_type=MESH,
        )

    def kv_copy(k, source, c, target):
        return remote(
            kv.at[:, c, source],
            kv.at[:, c, k],
            kv_send.at[k - 1],
            kv_recv.at[k - 1, c],
            "seq",
            target,
        )

    def q_copy(k, source, g, target):
        duo = pl.ds(2 * g, 2)
        return remote(
            qs.at[duo, source],
            qs.at[duo, k],
            q_send.at[k - 1],
            q_recv.at[k - 1, g],
            "seq",
            target,
        )

    def og_copy(k, source, p, target):
        part = pl.ds(p * piece, piece)
        return remote(
            og.at[source, part, cols(lane, width)],
            og.at[k, part, cols(lane, width)],
            og_send.at[k - 1],
            og_recv.at[k - 1, p],
            "seq",
            target,
        )

    def peer_copy(k, j, shard, p, target):
        part = og.at[k, pl.ds(p * piece, piece), cols(shard, width)]
        return remote(part, part, lane_send.at[k], peer_recv.at[k, p, j], "head", target)

    def twin_copy(k, shard, p):
        part = og.at[k, pl.ds(p * piece, piece), cols(shard, width)]
        return remote(part, part, lane_send.at[k], twin_recv.at[k], "head", twin)

    def part_copy(k, target):
        return remote(
            part_out.at[:, k - 1],
            part_in.at[:, k - 1],
            part_send.at[k - 1],
            part_recv.at[k - 1],
            "seq",
            target,
        )

    def term_copy(k, c, target):
        return remote(
            term.at[c - keyed, k - 1],
            back.at[c - keyed, k - 1],
            term_send.at[k - 1],
            term_recv.at[k - 1, c - keyed],
            "seq",
            target,
        )

    groups = [(0, keyed - 2), (keyed - 2, keyed - 1), (keyed - 1, keyed), (keyed, heads)]

    def group_of(c):
        return [low <= c < high for low, high in groups].index(True)

    def stat_copy(k, group, target):
        low, high = groups[group]
        some_heads = pl.ds(low, high - low)
        return remote(
            stat_out.at[some_heads, k - 1],
            stat_in.at[some_heads, k - 1],
            stat_send.at[k - 1],
            stat_recv.at[k - 1, group],
            "seq",
            target,
        )

    barrier = pltpu.get_barrier_semaphore()
    arrivals = jnp.int32(2 + len(peers))
    for peer in [twin] + peers:
        pl.semaphore_signal(barrier, inc=1, device_id={"head": peer}, device_id_type=MESH)
    pl.semaphore_signal(barrier, inc=1, device_id={"seq": pair}, device_id_type=MESH)
    for present, target in (
        (has_up, up),
        (has_down, down),
        (has_far, me - half),
        (has_near, me + half),
        (has_other, other),
    ):
        arrivals = arrivals + present.astype(jnp.int32)

        @pl.when(present)
        def _():
            pl.semaphore_signal(barrier, inc=1, device_id={"seq": target}, device_id_type=MESH)

    load_og = pltpu.make_async_copy(og_hbm, og.at[0, :, cols(lane, width)], load_sem.at[0])

    def load_kv(c):
        for j, source in enumerate((k_hbm, v_hbm)):
            pltpu.make_async_copy(
                source.at[:, cols(c, HDIM)],
                kv.at[j, c, 0],
                load_sem.at[1 if c < EARLY else 2],
            ).start()

    load_og.start()
    for c in range(EARLY):
        load_kv(c)

    pl.semaphore_wait(barrier, arrivals)

    def gather_start(k, p):
        for j, peer in enumerate(peers):
            peer_copy(k, j, lane, p, peer).start()
        twin_copy(k, lane, p).start()

    def gather_pass(k):
        for p in range(2):
            for j in range(len(peers)):
                shard = lax.rem(lane + lanes - 2 * (j + 1), lanes)
                peer_copy(k, j, shard, p, lane).wait_recv()
                twin_copy(k, shard, p).start()

    def gather_end(k):
        settle(og.at[k, :, pl.ds(0, lanes // 2 * width)], twin_recv.at[k]).wait()

    def send_kv(c):
        ready("early" if c < EARLY else "late")

        @pl.when(has_up)
        def _():
            kv_copy(2, 0, c, up).start()

        @pl.when(even)
        def _():
            kv_copy(3, 0, c, pair).start()

    def send_q(c):
        ready("query")

        @pl.when(has_down)
        def _():
            q_copy(2, 0, c, down).start()

    def side_q(c):
        ready("query")

        @pl.when(odd)
        def _():
            q_copy(3, 0, c, pair).start()

    def relay_kv(c):
        @pl.when(has_down)
        def _():
            kv_copy(2, 0, c, up).wait_recv()

        @pl.when(has_both)
        def _():
            kv_copy(1, 2, c, up).start()

        @pl.when(odd_and_down)
        def _():
            kv_copy(3, 2, c, pair).start()

    def relay_q(c):
        @pl.when(has_up)
        def _():
            q_copy(2, 0, c, down).wait_recv()

        @pl.when(has_both)
        def _():
            q_copy(1, 2, c, down).start()

        @pl.when(even_and_up)
        def _():
            q_copy(3, 2, c, pair).start()

    tables = [
        pltpu.make_async_copy(table_hbm, table_ref, load_sem.at[5]),
        pltpu.make_async_copy(active_hbm, active_ref, load_sem.at[6]),
    ]
    def load_proj(t):
        part = pl.ds(t * 2 * HDIM, 2 * HDIM)
        return pltpu.make_async_copy(proj_hbm.at[part], proj.at[part], load_sem.at[4])

    def settle(ref, sem):
        return pltpu.make_async_copy(ref, ref, sem)

    pending = {
        "early": [settle(kv.at[:, pl.ds(0, EARLY), 0], load_sem.at[1])],
        "late": [settle(kv.at[:, pl.ds(EARLY, heads - EARLY), 0], load_sem.at[2])],
        "query": [settle(qs.at[:, 0], load_sem.at[3])],
        "proj": [settle(proj, load_sem.at[4])],
        "table": tables,
    }

    def ready(*names):
        for name in names:
            for copy in pending.pop(name, ()):
                copy.wait()

    here = {0: me >= 0, 1: has_near, 2: has_up, 3: even_or_up}
    reach = {1: has_far, 2: has_down, 3: odd_or_down}
    def fetch():
        for c in range(EARLY, heads):
            load_kv(c)

        for c in range(heads):
            pltpu.make_async_copy(
                q_hbm.at[:, cols(c, HDIM)], qs.at[c, 0], load_sem.at[3]
            ).start()

        for copy in tables:
            copy.start()

    def clear():
        for k in range(1, SETS):

            @pl.when(jnp.logical_not(reach[k]))
            def _():
                @pl.loop(0, keyed)
                def _(c):
                    for j in range(2):
                        kv[j, c, k] = jnp.zeros((rows, HDIM), BF16)

                for c in range(ASKED):
                    part_in[c, k - 1] = jnp.full((3, rows), -FAR, F32)

            @pl.when(jnp.logical_not(here[k]))
            def _():
                @pl.loop(0, heads)
                def _(c):
                    qs[c, k] = jnp.zeros((rows, HDIM), BF16)
                    gs[c, k] = jnp.zeros((rows, HDIM), BF16)
                    stat_in[c, k - 1] = jnp.full((2, rows), FAR, F32)

        for k, present in ((1, has_both), (2, has_down), (3, jnp.logical_or(odd, has_up))):

            @pl.when(jnp.logical_not(present))
            def _():
                for c in range(ASKED):
                    back[c, k - 1] = jnp.zeros((HDIM, rows), BF16)

    load_og.wait()
    for p in range(2):
        gather_start(0, p)

        @pl.when(has_down)
        def _():
            og_copy(2, 0, p, down).start()

        @pl.when(odd)
        def _():
            og_copy(3, 0, p, pair).start()

    for c in range(EARLY):
        send_kv(c)

    fetch()

    def project(k, low, high):
        for t in range(low // 2, high // 2):
            tile = proj[cols(t, 2 * HDIM), :]
            grad = dot(og[k], tile, ((1,), (1,))).astype(BF16)
            gs[2 * t, k] = grad[:, :HDIM]
            gs[2 * t + 1, k] = grad[:, HDIM:]

    key_index = lax.broadcasted_iota(jnp.int32, (rows, rows), 0)
    query_index = lax.broadcasted_iota(jnp.int32, (rows, rows), 1)

    def attend(c):
        ready("query", "table")
        for k in (1, 3):

            @pl.when(reach[k])
            def _():
                kv_copy(k, 0, c, me).wait_recv()

        query, grad = qs[c, 0], gs[c, 0]
        tops, totals, sums, exps, prob_grads = [], [], [], [], []
        for k in range(SETS):
            logits = dot(kv[0, c, k], query, ((1,), (1,))) * scale2
            if k == 0:
                logits = jnp.where(key_index <= query_index, logits, -FAR)
            prob_grads.append(dot(kv[1, c, k], grad, ((1,), (1,))))
            best = jnp.max(logits, axis=0, keepdims=True)
            exps.append(jnp.exp2(logits - best))
            totals.append(jnp.sum(exps[k], axis=0, keepdims=True))
            sums.append(jnp.sum(exps[k] * prob_grads[k], axis=0, keepdims=True))
            if k:
                usable = jnp.logical_and(
                    table_ref[k - 1, c] * active_ref[0, k - 1] > 0, me >= count // 2**k
                )
                best = best + jnp.where(usable, 0.0, -FAR).astype(F32)
            tops.append(best)
        top = functools.reduce(jnp.maximum, tops)
        shares = [jnp.exp2(x - top) for x in tops]
        total = sum(share * x for share, x in zip(shares, totals))
        inverse = 1.0 / total
        delta = sum(share * x for share, x in zip(shares, sums)) * inverse
        norm = top + jnp.log2(total)
        for k in range(1, SETS):
            hidden = jnp.where(active_ref[0, k - 1] > 0, 0.0, FAR).astype(F32)
            stat_out[c, k - 1] = jnp.concatenate([norm + hidden, delta], axis=0)

        probs = exps[0] * (shares[0] * inverse)
        dlogit = (probs * (prob_grads[0] - delta)).astype(BF16)
        terms = dot(kv[0, c, 0], dlogit, ((0,), (0,)))
        for k in range(1, SETS):
            part = (exps[k] * (prob_grads[k] - delta)).astype(BF16)
            terms = terms + dot(kv[0, c, k], part, ((0,), (0,))) * (shares[k] * inverse)
        own[0, c] = dot(dlogit, query, ((1,), (0,))) * scale
        own[1, c] = dot(probs.astype(BF16), grad, ((1,), (0,)))
        dq_ref[:, cols(c, HDIM)] = (terms * scale).T.astype(BF16)
        tell(c)

    def tell(c):
        group = group_of(c)
        if c + 1 < groups[group][1]:
            return

        for k, go, span in ((1, has_far, half), (2, has_down, quarter), (3, odd_or_down, eighth)):

            @pl.when(go)
            def _():
                stat_copy(k, group, me - span).start()

    heard = set()

    def hear(group):
        if group in heard:
            return

        heard.add(group)
        for k, span in ((1, half), (2, quarter), (3, eighth)):

            @pl.when(here[k])
            def _():
                stat_copy(k, group, me + span).wait_recv()

    asked_for = set()

    def meet(g):
        if g in asked_for:
            return

        asked_for.add(g)
        for k in (1, 3):

            @pl.when(here[k])
            def _():
                q_copy(k, 0, g, me).wait_recv()

    def collect(c):
        queries = qs[c, 1:].reshape(SECTIONS * rows, HDIM)
        grads = gs[c, 1:].reshape(SECTIONS * rows, HDIM)
        raw = dot(kv[0, c, 0], queries, ((1,), (1,))) * scale2
        prob_grad = dot(kv[1, c, 0], grads, ((1,), (1,)))
        weights, dlogits = [], []
        for k in range(1, SETS):
            part = slice((k - 1) * rows, k * rows)
            hidden = jnp.where(table_ref[k - 1, c] > 0, 0.0, FAR).astype(F32)
            probs = jnp.exp2(raw[:, part] - (stat_in[c, k - 1, 0:1] + hidden))
            weights.append(probs.astype(BF16))
            dlogits.append((probs * (prob_grad[:, part] - stat_in[c, k - 1, 1:2])).astype(BF16))
        key = dot(jnp.concatenate(dlogits, axis=1), queries, ((1,), (0,)))
        value = dot(jnp.concatenate(weights, axis=1), grads, ((1,), (0,)))
        dk_ref[:, cols(c, HDIM)] = (own[0, c] + key * scale).astype(BF16)
        dv_ref[:, cols(c, HDIM)] = (own[1, c] + value).astype(BF16)

    def finish(c):
        hear(group_of(c))
        meet(c // 2)
        collect(c)

    def arrive(k, p):
        @pl.when(here[k])
        def _():
            og_copy(k, 0, p, me).wait_recv()
            if k == 2:

                @pl.when(has_both)
                def _():
                    og_copy(1, 2, p, down).start()

                @pl.when(even)
                def _():
                    og_copy(3, 2, p, pair).start()

            gather_start(k, p)

    def hand_on(k):
        @pl.when(here[k])
        def _():
            gather_pass(k)

    def take(k, low=0, high=heads):
        ready("proj")

        @pl.when(here[k])
        def _():
            gather_end(k)
            project(k, low, high)

    def some(k):
        take(k, keyed, heads)

    def rest(k):
        @pl.when(here[k])
        def _():
            project(k, 0, keyed)

    def ask(first):
        ready("late", "table")
        for c in range(first, heads):
            if c % 2 == 0:
                meet(c // 2)

        for c in range(first, heads):
            ask_one(c)

        for k, span in ((1, half), (2, quarter), (3, eighth)):

            @pl.when(here[k])
            def _():
                part_copy(k, me + span).start()

    def ask_one(c):
        raw = dot(kv[0, c, 0], qs[c].reshape(SETS * rows, HDIM), ((1,), (1,))) * scale2
        prob_grad = dot(kv[1, c, 0], gs[c].reshape(SETS * rows, HDIM), ((1,), (1,)))
        for k in range(SETS):
            part = slice(k * rows, (k + 1) * rows)
            logits = raw[:, part]
            if k == 0:
                logits = jnp.where(key_index <= query_index, logits, -FAR)
            top = jnp.max(logits, axis=0, keepdims=True)
            exps = jnp.exp2(logits - top)
            total = jnp.sum(exps, axis=0, keepdims=True)
            weighted = jnp.sum(exps * prob_grad[:, part], axis=0, keepdims=True)
            if k == 0:
                part_own[c - keyed] = jnp.concatenate([top, total, weighted], axis=0)
            else:
                top = top + jnp.where(table_ref[k - 1, c] > 0, 0.0, -FAR).astype(F32)
                part_out[c - keyed, k - 1] = jnp.concatenate([top, total, weighted], axis=0)
    def combine(first):
        for k in range(1, SETS):

            @pl.when(reach[k])
            def _():
                part_copy(k, me).wait_recv()

        for c in range(first, heads):
            combine_one(c)

        tell(heads - 1)

    def combine_one(c):
        h = c - keyed
        tops, parts = [part_own[h, 0:1]], [(part_own[h, 1:2], part_own[h, 2:3])]
        for k in range(1, SETS):
            usable = jnp.logical_and(active_ref[0, k - 1] > 0, me >= count // 2**k)
            hidden = jnp.where(usable, 0.0, -FAR).astype(F32)
            tops.append(part_in[h, k - 1, 0:1] + hidden)
            sums = part_in[h, k - 1]
            parts.append((jnp.where(usable, sums[1:2], 0.0), jnp.where(usable, sums[2:3], 0.0)))
        top = functools.reduce(jnp.maximum, tops)
        shares = [jnp.exp2(x - top) for x in tops]
        total = sum(share * part[0] for share, part in zip(shares, parts))
        delta = sum(share * part[1] for share, part in zip(shares, parts)) / total
        norm = top + jnp.log2(total)
        stat_own[h] = jnp.concatenate([norm, delta], axis=0)
        for k in range(1, SETS):
            hidden = jnp.where(active_ref[0, k - 1] > 0, 0.0, FAR).astype(F32)
            stat_out[c, k - 1] = jnp.concatenate([norm + hidden, delta], axis=0)

    def answer(c):
        hear(group_of(c))
        h = c - keyed
        queries = qs[c].reshape(SETS * rows, HDIM)
        grads = gs[c].reshape(SETS * rows, HDIM)
        raw = dot(kv[0, c, 0], queries, ((1,), (1,))) * scale2
        prob_grad = dot(kv[1, c, 0], grads, ((1,), (1,)))
        weights, dlogits = [], []
        for k in range(SETS):
            part = slice(k * rows, (k + 1) * rows)
            logits = raw[:, part]
            if k == 0:
                logits = jnp.where(key_index <= query_index, logits, -FAR)
                norm, delta = stat_own[h, 0:1], stat_own[h, 1:2]
            else:
                hidden = jnp.where(table_ref[k - 1, c] > 0, 0.0, FAR).astype(F32)
                norm, delta = stat_in[c, k - 1, 0:1] + hidden, stat_in[c, k - 1, 1:2]
            probs = jnp.exp2(logits - norm)
            weights.append(probs.astype(BF16))
            dlogits.append((probs * (prob_grad[:, part] - delta)).astype(BF16))
        dlogit = jnp.concatenate(dlogits, axis=1)
        terms = dot(kv[0, c, 0], dlogit, ((0,), (0,))) * scale
        held[h] = terms[:, :rows]
        for k in range(1, SETS):
            term[h, k - 1] = terms[:, k * rows : (k + 1) * rows].astype(BF16)

        @pl.when(has_near)
        def _():
            term_copy(1, c, up).start()

        @pl.when(even_or_up)
        def _():
            term_copy(3, c, pair).start()

        dk_ref[:, cols(c, HDIM)] = (dot(dlogit, queries, ((1,), (0,))) * scale).astype(BF16)
        weight = jnp.concatenate(weights, axis=1)
        dv_ref[:, cols(c, HDIM)] = dot(weight, grads, ((1,), (0,))).astype(BF16)

    def merge(c):
        h = c - keyed

        @pl.when(has_both)
        def _():
            term_copy(1, c, me).wait_recv()

        @pl.when(jnp.logical_or(odd, has_up))
        def _():
            term_copy(3, c, me).wait_recv()

        @pl.when(has_up)
        def _():
            side = jnp.where(even, back[h, 2].astype(F32), 0.0)
            total = term[h, 1].astype(F32) + back[h, 0].astype(F32) + side
            term[h, 1] = total.astype(BF16)
            term_copy(2, c, up).start()

    def close(c):
        h = c - keyed

        @pl.when(has_down)
        def _():
            term_copy(2, c, me).wait_recv()

        side = jnp.where(odd, back[h, 2].astype(F32), 0.0)
        total = held[h] + back[h, 1].astype(F32) + side
        dq_ref[:, cols(c, HDIM)] = total.T.astype(BF16)

    plan = []
    for low, high, timed in (
        (EARLY, keyed, ((send_kv, -23.33, 6.09),)),
        (
            0,
            keyed,
            (
                (relay_kv, -26.96, 13.35),
                (attend, 20.51, 7.47),
                (finish, 60.00, 11.97),
            ),
        ),
        (
            0,
            keyed // 2,
            (
                (side_q, -35.62, 6.80),
                (send_q, -20.90, 13.31),
                (relay_q, 16.37, 10.96),
            ),
        ),
        (
            keyed // 2,
            heads // 2,
            (
                (side_q, -45.00, 2.05),
                (send_q, -34.11, 178.66),
                (relay_q, -14.51, 42700.55),
            ),
        ),
        (
            keyed,
            heads,
            (
                (answer, 57.25, 0.32),
                (merge, 60.00, 25.48),
                (close, 119.40, 2041502.52),
            ),
        ),
    ):
        for action, start, step in timed:
            for c in range(low, high):
                plan.append((start + step * (c - low), functools.partial(action, c)))

    for due, action, *where in (
        (-27.93, arrive, 2, 0),
        (-24.44, arrive, 2, 1),
        (-23.63, hand_on, 0),
        (-17.30, arrive, 3, 0),
        (-10.64, hand_on, 2),
        (-5.73, take, 0),
        (-5.70, arrive, 3, 1),
        (4.22, take, 2),
        (10.57, arrive, 1, 0),
        (14.73, arrive, 1, 1),
        (17.82, hand_on, 3),
        (19.08, some, 3),
        (20.89, rest, 3),
        (21.27, hand_on, 1),
        (24.07, some, 1),
        (26.23, ask, keyed),
        (36.01, rest, 1),
        (37.92, combine, keyed),
    ):
        plan.append((due, functools.partial(action, *where)))

    for t in range(heads // 2):
        plan.append((-27.924 + t * 0.001, load_proj(t).start))

    plan.append((-27.918, clear))
    plan.sort(key=lambda entry: entry[0])
    for _, action in plan:
        action()

    def drain(present, ref, sem):
        @pl.when(present)
        def _():
            settle(ref, sem).wait()

    always = me >= 0
    odd_or_up = jnp.logical_or(odd, has_up)
    drain(always, og.at[0, :, pl.ds(0, (lanes - 1) * width)], lane_send.at[0])
    for k, kv_sent, q_sent, term_sent in (
        (1, has_both, has_both, has_near),
        (2, has_up, has_down, has_up),
        (3, jnp.logical_or(even, has_down), odd_or_up, even_or_up),
    ):
        drain(here[k], og.at[k, :, pl.ds(0, (lanes - 1) * width)], lane_send.at[k])
        drain(q_sent, og.at[0, :, pl.ds(0, width)], og_send.at[k - 1])
        drain(q_sent, qs.at[:, k], q_send.at[k - 1])
        drain(kv_sent, kv.at[:, pl.ds(0, keyed), k], kv_send.at[k - 1])
        drain(reach[k], stat_out.at[:, k - 1], stat_send.at[k - 1])
        drain(here[k], part_out.at[:, k - 1], part_send.at[k - 1])
        drain(term_sent, term.at[:, k - 1], term_send.at[k - 1])


def publish_kernel(*refs):
    number = (len(refs) - 1) // 2
    copies = [
        pltpu.make_async_copy(refs[a], refs[number + a], refs[-1].at[a]) for a in range(number)
    ]
    for copy in copies:
        copy.start()
    for copy in copies:
        copy.wait()


def publish(arrays):
    number = len(arrays)
    held = [pltpu.with_memory_space_constraint(a, pltpu.VMEM) for a in arrays]
    return pl.pallas_call(
        publish_kernel,
        out_shape=[jax.ShapeDtypeStruct(a.shape, a.dtype) for a in arrays],
        in_specs=[pl.BlockSpec(memory_space=pltpu.VMEM)] * number,
        out_specs=[pl.BlockSpec(memory_space=pl.ANY)] * number,
        scratch_shapes=[pltpu.SemaphoreType.DMA((number,))],
        compiler_params=pltpu.CompilerParams(vmem_limit_bytes=2**20),
    )(*held)


def body(count, lanes, queries, key_rows, value_rows, out_grad, out_proj, table, active):
    rows, columns = queries.shape
    heads = columns // HDIM
    vmem = pl.BlockSpec(memory_space=pltpu.VMEM)
    hbm = pl.BlockSpec(memory_space=pl.ANY)
    dma = pltpu.SemaphoreType.DMA
    grads = pl.pallas_call(
        functools.partial(kernel, count, lanes),
        out_shape=[pltpu.VMEM((rows, columns), BF16)] * 3,
        in_specs=[hbm] * 7,
        out_specs=[vmem] * 3,
        scratch_shapes=[
            pltpu.VMEM((2, heads, SETS, rows, HDIM), BF16),
            pltpu.VMEM((heads, SETS, rows, HDIM), BF16),
            pltpu.VMEM((heads, SETS, rows, HDIM), BF16),
            pltpu.VMEM((SETS, rows, out_proj.shape[1]), BF16),
            pltpu.VMEM(out_proj.shape, BF16),
            pltpu.VMEM((2, heads, rows, HDIM), F32),
            pltpu.VMEM((heads, SECTIONS, 2, rows), F32),
            pltpu.VMEM((heads, SECTIONS, 2, rows), F32),
            pltpu.VMEM((ASKED, 3, rows), F32),
            pltpu.VMEM((ASKED, SECTIONS, 3, rows), F32),
            pltpu.VMEM((ASKED, SECTIONS, 3, rows), F32),
            pltpu.VMEM((ASKED, 2, rows), F32),
            pltpu.VMEM((ASKED, HDIM, rows), F32),
            pltpu.VMEM((ASKED, SECTIONS, HDIM, rows), BF16),
            pltpu.VMEM((ASKED, SECTIONS, HDIM, rows), BF16),
            pltpu.SMEM((SECTIONS, heads), jnp.int32),
            pltpu.SMEM((1, SECTIONS), jnp.int32),
            dma((7,)),
            dma((SECTIONS,)),
            dma((SECTIONS, heads - ASKED)),
            dma((SECTIONS,)),
            dma((SECTIONS, heads // 2)),
            dma((SECTIONS,)),
            dma((SECTIONS, 2)),
            dma((SETS,)),
            dma((SETS, 2, max(1, lanes // 2 - 1))),
            dma((SETS,)),
            dma((SECTIONS,)),
            dma((SECTIONS, 4)),
            dma((SECTIONS,)),
            dma((SECTIONS,)),
            dma((SECTIONS,)),
            dma((SECTIONS, ASKED)),
        ],
        compiler_params=pltpu.CompilerParams(
            collective_id=0, has_side_effects=True, vmem_limit_bytes=60 * 2**20
        ),
    )(queries, key_rows, value_rows, out_grad, out_proj, table.T, active)
    return tuple(publish(grads))


def solution(mesh):
    return jax.shard_map(
        functools.partial(body, mesh.shape["seq"], mesh.shape["head"]),
        mesh=mesh,
        in_specs=(
            P("seq", "head"),
            P("seq", "head"),
            P("seq", "head"),
            P("seq", "head"),
            P("head", None),
            P("head", None),
            P("seq", None),
        ),
        out_specs=(P("seq", "head"), P("seq", "head"), P("seq", "head")),
        check_vma=False,
    )
```
